32 devices in a mesh: span: 32 (over z, y, x, core).
Axes of the slice: x: 2, y: 2, z: 4, core: 2. Of those that a mesh axis runs over, the one named last changes fastest.
Arguments:
- random_slabs: bfloat16 [1024, 4, 3, 2048], P('span'), may hold values from -6 to 6
- span_weights: float32 [513], replicated, may hold values from 0.1 to 2
- wall_filter: bfloat16 [2048, 2048], replicated, may hold values from -0.125 to 0.125
- prev_state: float32 [1024, 3, 2048], P('span'), may hold values from -6 to 6
- time_scale: float32 [3, 2048], replicated, may hold values from 1 to 32
- mean_velocity: float32 [2048], replicated, may hold values from 0 to 2
- lund_diag: float32 [3, 2048], replicated, may hold values from 0.3 to 3
- lund_off: float32 [3, 2048], replicated, may hold values from -1 to 1
Outputs:
- velocity: bfloat16 [1024, 4, 3, 2048], P('span')
- new_state: float32 [1024, 3, 2048], P('span')
The draws below stay inside these ranges and needn't reach their ends.
All inputs are finite; a program needn't handle non-finite values.
Results may differ from the reference program's by a relative error of at most 0.0051.
Values may be sent and summed in bfloat16 or wider, within the bound.
A program may use at most 128 MiB of HBM per device.

```python
import math
import jax
import jax.numpy as jnp
from jax import lax

NY = 2048
PLANES = 4
NZ = 1024
HALF = 256


def draw_span_weights(key, part):
    offsets = jnp.arange(-HALF, HALF + 1).astype(jnp.float32)
    spread = jnp.float32(HALF)
    envelope = jnp.exp(-jnp.pi * offsets * offsets / (2.0 * spread * spread))
    factor = jnp.exp(jax.random.uniform(key, (2 * HALF + 1,), jnp.float32, math.log(0.5), math.log(2.0)))
    return envelope * factor


def steps_of(rng, shape, cuts, smallest, top_value):
    factor_of, own = 1.0, jax.random.fold_in(rng, 6)
    for position, shards_of in cuts:
        steps = jnp.exp(jax.random.uniform(jax.random.fold_in(own, position), (shards_of,), jnp.float32, smallest / len(cuts), top_value / len(cuts)))
        factor_of = factor_of * jnp.repeat(steps, shape[position] // shards_of).reshape([-1 if axis == position else 1 for axis in range(len(shape))])
    return factor_of


def bell_draw(rng, extent, scale, bound, shards=(), kind=jnp.bfloat16):
    level = steps_of(rng, extent, shards, -0.22, 0.18) if shards else 1.0
    result = jax.random.normal(rng, extent, jnp.float32) * scale * level
    return jnp.minimum(jnp.maximum(result, -bound), bound).astype(kind)


def setup_inputs(seed: int = 0) -> dict:
    key_list = jax.random.split(jax.random.key(seed), 9)
    return {
        "random_slabs": bell_draw(key_list[0], (NZ, PLANES, 3, NY), 1.0, 6.0, ((0, 32),)),
        "span_weights": draw_span_weights(jax.random.fold_in(key_list[8], 71), 0),
        "wall_filter": bell_draw(key_list[2], (NY, NY), NY ** -0.5, 0.125),
        "prev_state": bell_draw(key_list[3], (NZ, 3, NY), 1.0, 6.0, ((0, 32),), jnp.float32),
        "time_scale": jnp.clip(jnp.exp(jax.random.uniform(key_list[4], (3, NY), jnp.float32, math.log(1.0), math.log(32.0))), 1.0, 32.0),
        "mean_velocity": jnp.clip(jax.random.uniform(key_list[5], (NY,), jnp.float32, 0.0, 2.0), 0.0, 2.0),
        "lund_diag": jnp.clip(jnp.exp(jax.random.uniform(key_list[6], (3, NY), jnp.float32, math.log(0.3), math.log(3.0))), 0.3, 3.0),
        "lund_off": jnp.clip(jax.random.uniform(key_list[7], (3, NY), jnp.float32, -1.0, 1.0), -1.0, 1.0),
    }


def normalized_taps(span_weights):
    norm = jnp.sqrt(jnp.sum(span_weights * span_weights))
    return (span_weights / norm).astype(jnp.bfloat16)

def reference(random_slabs, span_weights, wall_filter, prev_state, time_scale, mean_velocity, lund_diag, lund_off):
    total = random_slabs.shape[0]
    taps = lax.optimization_barrier(normalized_taps(span_weights)).astype(jnp.float32)
    middle = jnp.zeros((total - 2 * HALF - 1,), jnp.float32)
    kernel = jnp.concatenate([taps[HALF:], middle, taps[:HALF]])
    kernel_hat = jnp.conj(jnp.fft.rfft(kernel))
    slabs = random_slabs.reshape(total, PLANES * 3, NY).transpose(1, 0, 2)
    wall_wide = wall_filter.astype(jnp.float32)

    def one_slab(slab):
        spectrum = jnp.fft.rfft(slab.astype(jnp.float32), axis=0)
        spanned = jnp.fft.irfft(spectrum * kernel_hat[:, None], n=total, axis=0)
        spanned = lax.optimization_barrier(spanned.astype(jnp.bfloat16)).astype(jnp.float32)
        return jnp.dot(spanned, wall_wide.T, precision=lax.Precision.HIGHEST)
    filtered = lax.map(one_slab, slabs).reshape(PLANES, 3, total, NY)
    decay = jnp.exp(-jnp.pi / (2.0 * time_scale))[:, None, :]
    inject = jnp.sqrt(1.0 - jnp.exp(-jnp.pi / time_scale))[:, None, :]

    def advance(state, plane):
        state = decay * state + inject * plane
        return (state, state)
    final, fluct = lax.scan(advance, prev_state.transpose(1, 0, 2), filtered)
    along = fluct[:, 0]
    normal = fluct[:, 1]
    spanwise = fluct[:, 2]
    first = mean_velocity + lund_diag[0] * along
    second = lund_off[0] * along + lund_diag[1] * normal
    third = lund_off[1] * along + lund_off[2] * normal + lund_diag[2] * spanwise
    velocity = jnp.stack([first, second, third], axis=1).astype(jnp.bfloat16)
    return (velocity.transpose(2, 0, 1, 3), final.transpose(1, 0, 2))
```

```python
import functools

import jax
import jax.numpy as jnp
from jax import lax
from jax.experimental import pallas as pl
from jax.experimental.pallas import tpu as pltpu
from jax.sharding import PartitionSpec as P

LANES = 256
GRANT = 32 << 20
MESH = pl.DeviceIdType.MESH


def peer_at(step, me, count):
    away = count // 2 + (1 - 2 * (step % 2)) * ((step + 1) // 2)
    return lax.rem(me + away, count)


def exchange_kernel(
    count,
    rows,
    width,
    planes,
    kinds,
    slim,
    reach,
    slab_hbm,
    taps_hbm,
    wall_hbm,
    prev_hbm,
    scale_hbm,
    mean_hbm,
    diag_hbm,
    off_hbm,
    vel_ref,
    state_ref,
    slab,
    taps_ref,
    scale_ref,
    mean_ref,
    diag_ref,
    off_ref,
    x_ref,
    wide,
    summed,
    back,
    band,
    wall,
    early,
    along,
    normal,
    decay,
    inject,
    load_sem,
    slab_sem,
    out_sem,
    in_sem,
    back_out_sem,
    back_in_sem,
):
    me = lax.axis_index("span")
    blocks = count * rows // reach
    half = count // 2
    ours = me // half

    slab_loads = [
        pltpu.make_async_copy(slab_hbm.at[:, kind], slab.at[kind], slab_sem.at[kind])
        for kind in range(kinds)
    ]
    loads = [
        pltpu.make_async_copy(source, target, load_sem.at[at])
        for at, (source, target) in enumerate(
            (
                (taps_hbm, taps_ref),
                (scale_hbm, scale_ref),
                (mean_hbm, mean_ref),
                (diag_hbm, diag_ref),
                (off_hbm, off_ref),
                (prev_hbm, state_ref),
                (wall_hbm, wall),
            )
        )
    ]
    slab_loads[0].start()
    barrier = pltpu.get_barrier_semaphore()

    @pl.loop(0, count - 1)
    def _(step):
        pl.semaphore_signal(
            barrier, inc=1, device_id=(peer_at(step, me, count),), device_id_type=MESH
        )

    for load in slab_loads[1:]:
        load.start()
    for load in loads:
        load.start()

    def relayout(kind):
        slab_loads[kind].wait()
        for plane in range(planes):
            x_ref[kind, plane] = slab[kind, :, plane, :]

    relayout(0)
    pl.semaphore_wait(barrier, count - 1)

    side = width // slim // 2

    def columns(owner):
        place = owner % half
        start = pl.multiple_of((owner // half * side + place % side) * slim, slim)
        return place // side, pl.ds(start, slim)

    for part in range(kinds):
        if part:
            relayout(part)

        @pl.loop(0, count - 1)
        def _(step):
            peer = peer_at(step, me, count)
            plane, span = columns(peer)
            pltpu.make_async_remote_copy(
                src_ref=x_ref.at[part, plane, :, span],
                dst_ref=wide.at[part, me],
                send_sem=out_sem.at[part],
                recv_sem=in_sem.at[part],
                device_id=(peer,),
                device_id_type=MESH,
            ).start()

        plane, span = columns(me)
        pltpu.make_async_copy(
            x_ref.at[part, plane, :, span], wide.at[part, me], in_sem.at[part]
        ).start()

    for load in loads:
        load.wait()
    weights = jnp.concatenate(
        [taps_ref[...], jnp.zeros((3 * reach - taps_ref.shape[0],), jnp.float32)]
    ).reshape(1, 3 * reach)
    taps = weights / jnp.sqrt(jnp.sum(weights * weights))
    tall = jnp.broadcast_to(taps, (16, 3 * reach))
    line = lax.broadcasted_iota(jnp.int32, (16, 3 * reach), 0)
    for bit in range(4):
        tall = jnp.where((line // (1 << bit)) % 2 == 1, pltpu.roll(tall, 1 << bit, 1), tall)

    @pl.loop(0, reach // 16)
    def _(step):
        first = pl.multiple_of(step * 16, 16)
        rolled = pltpu.roll(tall, first, 1)
        band[pl.ds(first, 16), :] = rolled.astype(jnp.bfloat16)

    decay[...] = jnp.exp(-jnp.pi / (2.0 * scale_ref[...]))
    inject[...] = jnp.sqrt(1.0 - jnp.exp(-jnp.pi / scale_ref[...]))

    for part in range(kinds):
        pltpu.make_async_copy(wide.at[part], wide.at[part], in_sem.at[part]).wait()
        share = reach // rows
        for block in range(blocks):
            total = jnp.zeros((reach, slim), jnp.float32)
            for shift in range(3):
                source = (block - 1 + shift) % blocks
                chunk = wide[part, source * share : (source + 1) * share].reshape(reach, slim)
                total += jnp.dot(
                    band[:, shift * reach : (shift + 1) * reach],
                    chunk,
                    preferred_element_type=jnp.float32,
                )
            summed[part, block * share : (block + 1) * share] = total.astype(
                jnp.bfloat16
            ).reshape(share, rows, slim)

        plane, span = columns(me)

        @pl.loop(0, count - 1)
        def _(step):
            peer = peer_at(step, me, count)
            far = (peer // half + ours) % 2
            pltpu.make_async_remote_copy(
                src_ref=summed.at[part, peer],
                dst_ref=back.at[part, plane, :, span],
                send_sem=back_out_sem.at[part],
                recv_sem=back_in_sem.at[part, far],
                device_id=(peer,),
                device_id_type=MESH,
            ).start()

        pltpu.make_async_copy(
            summed.at[part, me], back.at[part, plane, :, span], back_in_sem.at[part, 0]
        ).start()

    def finish(part, at, filtered):
        one = pl.ds(part, 1)
        state = state_ref[part, :, at]
        values = []
        for plane in range(planes):
            state = decay[one, at] * state + inject[one, at] * filtered[plane]
            if part == 0:
                along[plane, :, at] = state
                value = mean_ref[:, at] + diag_ref[0:1, at] * state
            elif part == 1:
                normal[plane, :, at] = state
                value = off_ref[0:1, at] * along[plane, :, at] + diag_ref[1:2, at] * state
            else:
                value = (
                    off_ref[1:2, at] * along[plane, :, at]
                    + off_ref[2:3, at] * normal[plane, :, at]
                    + diag_ref[2:3, at] * state
                )
            values.append(value)
        state_ref[part, :, at] = state
        vel_ref[:, part, :, at] = jnp.stack(values, axis=1).astype(jnp.bfloat16)

    tile = min(256, width)
    for part in range(kinds):
        held = back.at[part]
        last = part == kinds - 1
        for far in range(2):
            first = pl.multiple_of((ours + far) % 2 * (width // 2), width // 2)
            span = pl.ds(first, width // 2)
            mine = held.at[:, :, 0 : width // 2]
            pltpu.make_async_copy(mine, mine, back_in_sem.at[part, far]).wait()
            if not last and far == 0:
                continue

            @pl.loop(0, width // tile)
            def _(step):
                at = pl.ds(pl.multiple_of(step * tile, tile), tile)
                reading = span if last else slice(None)
                filtered = lax.dot_general(
                    held[:, :, reading].reshape(planes * rows, -1),
                    wall[at, reading],
                    (((1,), (1,)), ((), ())),
                    preferred_element_type=jnp.float32,
                ).reshape(planes, rows, tile)
                if far == 0:
                    early[:, :, at] = filtered
                else:
                    if last:
                        filtered += early[:, :, at]
                    finish(part, at, filtered)

    for part in range(kinds):
        sent = wide.at[part, 0 : count - 1]
        pltpu.make_async_copy(sent, sent, out_sem.at[part]).wait()
        pltpu.make_async_copy(sent, sent, back_out_sem.at[part]).wait()


def fits(count, rows, planes, kinds, width, reach, slim):
    return (
        planes * width == count * slim
        and kinds == 3
        and width % (2 * slim) == 0
        and count % 2 == 0
        and rows % 16 == 0
        and reach % rows == 0
        and reach % 128 == 0
        and count * rows % reach == 0
        and count * rows // reach >= 3
    )


def exchanged(
    random_slabs,
    span_weights,
    wall_filter,
    prev_state,
    time_scale,
    mean_velocity,
    lund_diag,
    lund_off,
):
    count = lax.axis_size("span")
    rows, planes, kinds, width = random_slabs.shape
    reach = (span_weights.shape[0] - 1) // 2
    slim = LANES
    operands = (
        random_slabs.transpose(0, 2, 1, 3),
        span_weights,
        wall_filter,
        prev_state.transpose(1, 0, 2),
        time_scale,
        mean_velocity.reshape(1, width),
        lund_diag,
        lund_off,
    )
    operands = [pltpu.with_memory_space_constraint(each, pltpu.HBM) for each in operands]
    in_vmem = pl.BlockSpec(memory_space=pltpu.VMEM)
    in_hbm = pl.BlockSpec(memory_space=pltpu.HBM)
    fine = (kinds, width)
    velocity, state = pl.pallas_call(
        functools.partial(exchange_kernel, count, rows, width, planes, kinds, slim, reach),
        out_shape=(
            pltpu.VMEM((rows, kinds, planes, width), jnp.bfloat16),
            pltpu.VMEM((kinds, rows, width), jnp.float32),
        ),
        in_specs=[in_hbm] * len(operands),
        out_specs=(in_vmem, in_vmem),
        scratch_shapes=[
            pltpu.VMEM((kinds, rows, planes, width), jnp.bfloat16),
            pltpu.VMEM(span_weights.shape, jnp.float32),
            pltpu.VMEM(fine, jnp.float32),
            pltpu.VMEM((1, width), jnp.float32),
            pltpu.VMEM(fine, jnp.float32),
            pltpu.VMEM(fine, jnp.float32),
            pltpu.VMEM((kinds, planes, rows, width), jnp.bfloat16),
            pltpu.VMEM((kinds, count, rows, slim), jnp.bfloat16),
            pltpu.VMEM((kinds, count, rows, slim), jnp.bfloat16),
            pltpu.VMEM((kinds, planes, rows, width), jnp.bfloat16),
            pltpu.VMEM((reach, 3 * reach), jnp.bfloat16),
            pltpu.VMEM((width, width), jnp.bfloat16),
            pltpu.VMEM((planes, rows, width), jnp.float32),
            pltpu.VMEM((planes, rows, width), jnp.float32),
            pltpu.VMEM((planes, rows, width), jnp.float32),
            pltpu.VMEM(fine, jnp.float32),
            pltpu.VMEM(fine, jnp.float32),
            pltpu.SemaphoreType.DMA((7,)),
            pltpu.SemaphoreType.DMA((kinds,)),
            pltpu.SemaphoreType.DMA((kinds,)),
            pltpu.SemaphoreType.DMA((kinds,)),
            pltpu.SemaphoreType.DMA((kinds,)),
            pltpu.SemaphoreType.DMA((kinds, 2)),
        ],
        compiler_params=pltpu.CompilerParams(
            collective_id=0, has_side_effects=True, vmem_limit_bytes=GRANT
        ),
    )(*operands)
    return velocity.transpose(0, 2, 1, 3), state.transpose(1, 0, 2)


def from_partner(value, axis, bit):
    return lax.ppermute(value, axis, [(i, i ^ 1 << bit) for i in range(lax.axis_size(axis))])


def band_matrix(taps, height):
    reach = taps.shape[0]
    padded = jnp.concatenate([taps, jnp.zeros((height,), taps.dtype)])
    length = reach + height
    tiled = jnp.tile(padded, height)[: height * (length - 1)]
    return tiled.reshape(height, length - 1)


def butterfly(held, forward):
    count = lax.axis_size("span")
    device = lax.axis_index("span")
    levels = count.bit_length() - 1
    for level in range(levels - 1, -1, -1):
        groups, inner_first, targets, inner_last = held.shape
        halves = held.reshape(groups, inner_first, 2, targets // 2, inner_last)
        lower = halves[:, :, 0]
        higher = halves[:, :, 1]
        upper = device >> level & 1 == 1
        kept = jnp.where(upper, higher, lower)
        given = jnp.where(upper, lower, higher)
        if forward:
            taken = from_partner(given, "span", level)
        else:
            taken = from_partner(given, "span", level)
        first = jnp.where(upper, taken, kept)
        second = jnp.where(upper, kept, taken)
        held = jnp.stack([first, second], axis=1).reshape(
            groups * 2, inner_first, targets // 2, inner_last
        )
    return held


def body(
    random_slabs,
    span_weights,
    wall_filter,
    prev_state,
    time_scale,
    mean_velocity,
    lund_diag,
    lund_off,
):
    rows = random_slabs.shape[0]
    planes = random_slabs.shape[1]
    width = random_slabs.shape[3]
    columns = planes * 3 * width
    half = (span_weights.shape[0] - 1) // 2
    if fits(lax.axis_size("span"), rows, planes, 3, width, half, LANES):
        return exchanged(
            random_slabs,
            span_weights,
            wall_filter,
            prev_state,
            time_scale,
            mean_velocity,
            lund_diag,
            lund_off,
        )
    flat = random_slabs.reshape(rows, columns)
    scaling = jnp.sqrt(jnp.sum(span_weights * span_weights))
    taps = (span_weights / scaling).astype(jnp.bfloat16)
    reach = (span_weights.shape[0] - 1) // 2
    count = lax.axis_size("span")
    slim = columns // count
    held = butterfly(flat.reshape(1, rows, count, slim), True)
    total = rows * count
    whole = held.reshape(total, slim)
    height = min(512, total)
    matrix = band_matrix(taps, height)
    wrapped = jnp.concatenate([whole[total - reach :], whole, whole[:reach]], axis=0)

    def one_block(start):
        window = lax.dynamic_slice_in_dim(wrapped, start, height + 2 * reach, 0)
        return jnp.dot(matrix, window, preferred_element_type=jnp.float32)

    starts = jnp.arange(total // height) * height
    summed_cols = lax.map(one_block, starts).reshape(total, slim)
    rounded = summed_cols.astype(jnp.bfloat16)
    returned = butterfly(rounded.reshape(1, 1, count, rows * slim), False)
    spanned = returned.reshape(count, rows, slim).transpose(1, 0, 2).reshape(rows, planes, 3, width)
    filtered = lax.dot_general(
        spanned, wall_filter, (((3,), (1,)), ((), ())), preferred_element_type=jnp.float32
    )
    decay = jnp.exp(-jnp.pi / (2.0 * time_scale))
    inject = jnp.sqrt(1.0 - jnp.exp(-jnp.pi / time_scale))
    state = prev_state
    outputs = []
    for plane in range(planes):
        state = decay * state + inject * filtered[:, plane]
        along = state[:, 0]
        normal = state[:, 1]
        spanwise = state[:, 2]
        first = mean_velocity + lund_diag[0] * along
        second = lund_off[0] * along + lund_diag[1] * normal
        third = lund_off[1] * along + lund_off[2] * normal + lund_diag[2] * spanwise
        outputs.append(jnp.stack([first, second, third], axis=1).astype(jnp.bfloat16))
    velocity = jnp.stack(outputs, axis=1)
    return (velocity, state)


def solution(mesh):
    placed = (P("span", None, None, None), P(), P(), P("span", None, None), P(), P(), P(), P())
    return jax.shard_map(
        body,
        mesh=mesh,
        in_specs=placed,
        out_specs=(P("span", None, None, None), P("span", None, None)),
        check_vma=False,
    )
```

```python
import functools

import jax
import jax.numpy as jnp
from jax import lax
from jax.experimental import pallas as pl
from jax.experimental.pallas import tpu as pltpu
from jax.sharding import PartitionSpec as P

LANES = 256
GRANT = 44 << 20
MESH = pl.DeviceIdType.MESH


def peer_at(step, me, count, near_first=False):
    half, fourth, chips = count // 2, count // 4, count // 8
    if near_first:
        near, far = step + 1, step - half + 1
        away = step >= half - 1
    else:
        far, near = step // 2, step // 2 + 1
        away = step % 2 == 0
    side = 1 - me // half
    outer = side * 3 + far // fourth * (1 - 2 * side)
    there = outer * fourth + (me // 2 + far // 2) % chips * 2 + (me + far) % 2
    here = me // half * half + (me + near) % half
    return jnp.where(away, there, here)


def old_peer_at(step, me, count):
    away = count // 2 + (1 - 2 * (step % 2)) * ((step + 1) // 2)
    return lax.rem(me + away, count)


def exchange_kernel(
    count,
    rows,
    width,
    planes,
    kinds,
    slim,
    reach,
    slab_hbm,
    taps_hbm,
    wall_hbm,
    prev_hbm,
    scale_hbm,
    mean_hbm,
    diag_hbm,
    off_hbm,
    vel_ref,
    state_ref,
    slab,
    taps_ref,
    scale_ref,
    mean_ref,
    diag_ref,
    off_ref,
    x_ref,
    wide,
    summed,
    back,
    band,
    wall,
    turned,
    early_normal,
    early_spanwise,
    along,
    decay,
    inject,
    load_sem,
    slab_sem,
    out_sem,
    in_sem,
    back_out_sem,
    back_in_sem,
):
    me = lax.axis_index("span")
    blocks = count * rows // reach

    slab_loads = [
        pltpu.make_async_copy(slab_hbm.at[:, kind], slab.at[kind], slab_sem.at[kind])
        for kind in range(kinds)
    ]
    loads = [
        pltpu.make_async_copy(source, target, load_sem.at[at])
        for at, (source, target) in enumerate(
            (
                (taps_hbm, taps_ref),
                (scale_hbm, scale_ref),
                (mean_hbm, mean_ref),
                (diag_hbm, diag_ref),
                (off_hbm, off_ref),
                (prev_hbm, state_ref),
                (wall_hbm, wall),
            )
        )
    ]
    slab_loads[0].start()
    barrier = pltpu.get_barrier_semaphore()

    @pl.loop(0, count - 1)
    def _(step):
        pl.semaphore_signal(
            barrier, inc=1, device_id=(peer_at(step, me, count),), device_id_type=MESH
        )

    for load in slab_loads[1:]:
        load.start()
    for load in loads:
        load.start()

    def relayout(kind):
        slab_loads[kind].wait()
        for plane in range(planes):
            x_ref[kind, plane] = slab[kind, :, plane, :]

    relayout(0)
    pl.semaphore_wait(barrier, count - 1)

    half, chips = count // 2, count // 8

    def columns(owner):
        block = owner // half * chips + owner // 2 % chips
        plane = owner // (2 * chips) % 2 * 2 + owner % 2
        return plane, pl.ds(pl.multiple_of(block * slim, slim), slim)

    def batch(part, sender, receiver):
        late = (receiver // 2 - sender // 2 + chips) % chips
        far = jnp.where(sender // half == receiver // half, 0, 1 + late // (chips // 2))
        return (0, jnp.minimum(far, 1), far)[part]

    for part in range(kinds):
        if part:
            relayout(part)

        @pl.loop(0, count - 1)
        def _(step):
            peer = old_peer_at(step, me, count)
            plane, span = columns(peer)
            pltpu.make_async_remote_copy(
                src_ref=x_ref.at[part, plane, :, span],
                dst_ref=wide.at[part, me],
                send_sem=out_sem.at[part],
                recv_sem=in_sem.at[part],
                device_id=(peer,),
                device_id_type=MESH,
            ).start()

        plane, span = columns(me)
        pltpu.make_async_copy(
            x_ref.at[part, plane, :, span], wide.at[part, me], in_sem.at[part]
        ).start()

    for load in loads:
        load.wait()
    weights = jnp.concatenate(
        [taps_ref[...], jnp.zeros((3 * reach - taps_ref.shape[0],), jnp.float32)]
    ).reshape(1, 3 * reach)
    taps = weights / jnp.sqrt(jnp.sum(weights * weights))
    tall = jnp.broadcast_to(taps, (16, 3 * reach))
    line = lax.broadcasted_iota(jnp.int32, (16, 3 * reach), 0)
    for bit in range(4):
        tall = jnp.where((line // (1 << bit)) % 2 == 1, pltpu.roll(tall, 1 << bit, 1), tall)

    @pl.loop(0, reach // 16)
    def _(step):
        first = pl.multiple_of(step * 16, 16)
        rolled = pltpu.roll(tall, first, 1)
        band[pl.ds(first, 16), :] = rolled.astype(jnp.bfloat16)

    piece = min(256, width)

    @pl.loop(0, width // piece)
    def _(down):
        @pl.loop(0, width // piece)
        def _(over):
            here = pl.ds(pl.multiple_of(down * piece, piece), piece)
            there = pl.ds(pl.multiple_of(over * piece, piece), piece)
            turned[there, here] = wall[here, there].T

    decay[...] = jnp.exp(-jnp.pi / (2.0 * scale_ref[...]))
    inject[...] = jnp.sqrt(1.0 - jnp.exp(-jnp.pi / scale_ref[...]))

    for part in range(kinds):
        pltpu.make_async_copy(wide.at[part], wide.at[part], in_sem.at[part]).wait()
        share = reach // rows
        for block in range(blocks):
            total = jnp.zeros((reach, slim), jnp.float32)
            for shift in range(3):
                source = (block - 1 + shift) % blocks
                chunk = wide[part, source * share : (source + 1) * share].reshape(reach, slim)
                total += jnp.dot(
                    band[:, shift * reach : (shift + 1) * reach],
                    chunk,
                    preferred_element_type=jnp.float32,
                )
            summed[part, block * share : (block + 1) * share] = total.astype(
                jnp.bfloat16
            ).reshape(share, rows, slim)

        plane, span = columns(me)

        @pl.loop(0, count - 1)
        def _(step):
            peer = peer_at(step, me, count, True) if part == kinds - 1 else old_peer_at(step, me, count)
            arrival = batch(part, me, peer)
            pltpu.make_async_remote_copy(
                src_ref=summed.at[part, peer],
                dst_ref=back.at[part, plane, :, span],
                send_sem=back_out_sem.at[part],
                recv_sem=back_in_sem.at[part, arrival],
                device_id=(peer,),
                device_id_type=MESH,
            ).start()

        pltpu.make_async_copy(
            summed.at[part, me], back.at[part, plane, :, span], back_in_sem.at[part, 0]
        ).start()

    def advance(part, at, filtered):
        one = pl.ds(part, 1)
        state = state_ref[part, :, at]
        states = []
        for plane in range(planes):
            state = decay[one, at] * state + inject[one, at] * filtered[plane]
            states.append(state)
        state_ref[part, :, at] = state
        return states

    def put(part, at, values):
        vel_ref[:, part, :, at] = jnp.stack(values, axis=1).astype(jnp.bfloat16)

    def put_along(at, filtered):
        states = advance(0, at, filtered)
        for plane, state in enumerate(states):
            along[plane, :, at] = state
        put(0, at, [mean_ref[:, at] + diag_ref[0:1, at] * state for state in states])

    def put_normal(at, filtered):
        states = advance(1, at, filtered)
        values = []
        for plane, state in enumerate(states):
            first = along[plane, :, at]
            values.append(off_ref[0:1, at] * first + diag_ref[1:2, at] * state)
            along[plane, :, at] = off_ref[1:2, at] * first + off_ref[2:3, at] * state
        put(1, at, values)

    def base_spanwise(at, filtered):
        for plane, state in enumerate(advance(2, at, filtered)):
            along[plane, :, at] += diag_ref[2:3, at] * state

    def put_spanwise(at, filtered):
        extra = inject[2:3, at] * filtered[0]
        values = [along[0, :, at] + diag_ref[2:3, at] * extra]
        for plane in range(1, planes):
            extra = decay[2:3, at] * extra + inject[2:3, at] * filtered[plane]
            values.append(along[plane, :, at] + diag_ref[2:3, at] * extra)
        state_ref[2, :, at] += extra
        put(2, at, values)

    def arrived(part, arrival, pieces):
        piece = wide.at[part, 0:pieces]
        pltpu.make_async_copy(piece, piece, back_in_sem.at[part, arrival]).wait()

    def filtering(part, tile, chunks, early, finish):
        tile = min(tile, width)

        @pl.loop(0, width // tile)
        def _(step):
            at = pl.ds(pl.multiple_of(step * tile, tile), tile)
            total = None
            for first, size in chunks:
                reading = pl.ds(first, size)
                term = jnp.dot(
                    back[part, :, :, reading].reshape(planes * rows, size),
                    turned[reading, at],
                    preferred_element_type=jnp.float32,
                )
                total = term if total is None else total + term
            total = total.reshape(planes, rows, tile)
            if early is not None:
                total += early[:, :, at]
            finish(at, total)

    def keep(early):
        def run(at, filtered):
            early[:, :, at] = filtered

        return run

    ours = me // half
    near = [(pl.multiple_of(ours * (width // 2), width // 2), width // 2)]
    far = [(pl.multiple_of((1 - ours) * (width // 2), width // 2), width // 2)]
    turns = [(me // 2 - late + chips) % chips for late in range(chips)]
    late = [
        (pl.multiple_of(((1 - ours) * chips + turn) * slim, slim), slim) for turn in turns
    ]
    arrived(0, 0, count)
    filtering(0, 512, [(0, width)], None, put_along)
    arrived(1, 0, half)
    filtering(1, 1024, near, None, keep(early_normal))
    arrived(2, 0, half)
    filtering(2, 1024, near, None, keep(early_spanwise))
    arrived(1, 1, half)
    filtering(1, 1024, far, early_normal, put_normal)
    arrived(2, 1, half // 2)
    filtering(2, 1024, late[: chips // 2], early_spanwise, base_spanwise)
    arrived(2, 2, half // 2)
    filtering(2, 2048, late[chips // 2 :], None, put_spanwise)

    for part in range(kinds):
        sent = wide.at[part, 0 : count - 1]
        pltpu.make_async_copy(sent, sent, out_sem.at[part]).wait()
        pltpu.make_async_copy(sent, sent, back_out_sem.at[part]).wait()


def fits(count, rows, planes, kinds, width, reach, slim):
    return (
        planes * width == count * slim
        and kinds == 3
        and planes == 4
        and count % 16 == 0
        and rows % 16 == 0
        and reach % rows == 0
        and reach % 128 == 0
        and count * rows % reach == 0
        and count * rows // reach >= 3
    )


def exchanged(
    random_slabs,
    span_weights,
    wall_filter,
    prev_state,
    time_scale,
    mean_velocity,
    lund_diag,
    lund_off,
):
    count = lax.axis_size("span")
    rows, planes, kinds, width = random_slabs.shape
    reach = (span_weights.shape[0] - 1) // 2
    slim = LANES
    operands = (
        random_slabs.transpose(0, 2, 1, 3),
        span_weights,
        wall_filter,
        prev_state.transpose(1, 0, 2),
        time_scale,
        mean_velocity.reshape(1, width),
        lund_diag,
        lund_off,
    )
    operands = [pltpu.with_memory_space_constraint(each, pltpu.HBM) for each in operands]
    in_vmem = pl.BlockSpec(memory_space=pltpu.VMEM)
    in_hbm = pl.BlockSpec(memory_space=pltpu.HBM)
    fine = (kinds, width)
    velocity, state = pl.pallas_call(
        functools.partial(exchange_kernel, count, rows, width, planes, kinds, slim, reach),
        out_shape=(
            pltpu.VMEM((rows, kinds, planes, width), jnp.bfloat16),
            pltpu.VMEM((kinds, rows, width), jnp.float32),
        ),
        in_specs=[in_hbm] * len(operands),
        out_specs=(in_vmem, in_vmem),
        scratch_shapes=[
            pltpu.VMEM((kinds, rows, planes, width), jnp.bfloat16),
            pltpu.VMEM(span_weights.shape, jnp.float32),
            pltpu.VMEM(fine, jnp.float32),
            pltpu.VMEM((1, width), jnp.float32),
            pltpu.VMEM(fine, jnp.float32),
            pltpu.VMEM(fine, jnp.float32),
            pltpu.VMEM((kinds, planes, rows, width), jnp.bfloat16),
            pltpu.VMEM((kinds, count, rows, slim), jnp.bfloat16),
            pltpu.VMEM((kinds, count, rows, slim), jnp.bfloat16),
            pltpu.VMEM((kinds, planes, rows, width), jnp.bfloat16),
            pltpu.VMEM((reach, 3 * reach), jnp.bfloat16),
            pltpu.VMEM((width, width), jnp.bfloat16),
            pltpu.VMEM((width, width), jnp.bfloat16),
            pltpu.VMEM((planes, rows, width), jnp.float32),
            pltpu.VMEM((planes, rows, width), jnp.float32),
            pltpu.VMEM((planes, rows, width), jnp.float32),
            pltpu.VMEM(fine, jnp.float32),
            pltpu.VMEM(fine, jnp.float32),
            pltpu.SemaphoreType.DMA((7,)),
            pltpu.SemaphoreType.DMA((kinds,)),
            pltpu.SemaphoreType.DMA((kinds,)),
            pltpu.SemaphoreType.DMA((kinds,)),
            pltpu.SemaphoreType.DMA((kinds,)),
            pltpu.SemaphoreType.DMA((kinds, 3)),
        ],
        compiler_params=pltpu.CompilerParams(
            collective_id=0, has_side_effects=True, vmem_limit_bytes=GRANT
        ),
    )(*operands)
    return velocity.transpose(0, 2, 1, 3), state.transpose(1, 0, 2)


def from_partner(value, axis, bit):
    return lax.ppermute(value, axis, [(i, i ^ 1 << bit) for i in range(lax.axis_size(axis))])


def band_matrix(taps, height):
    reach = taps.shape[0]
    padded = jnp.concatenate([taps, jnp.zeros((height,), taps.dtype)])
    length = reach + height
    tiled = jnp.tile(padded, height)[: height * (length - 1)]
    return tiled.reshape(height, length - 1)


def butterfly(held, forward):
    count = lax.axis_size("span")
    device = lax.axis_index("span")
    levels = count.bit_length() - 1
    for level in range(levels - 1, -1, -1):
        groups, inner_first, targets, inner_last = held.shape
        halves = held.reshape(groups, inner_first, 2, targets // 2, inner_last)
        lower = halves[:, :, 0]
        higher = halves[:, :, 1]
        upper = device >> level & 1 == 1
        kept = jnp.where(upper, higher, lower)
        given = jnp.where(upper, lower, higher)
        if forward:
            taken = from_partner(given, "span", level)
        else:
            taken = from_partner(given, "span", level)
        first = jnp.where(upper, taken, kept)
        second = jnp.where(upper, kept, taken)
        held = jnp.stack([first, second], axis=1).reshape(
            groups * 2, inner_first, targets // 2, inner_last
        )
    return held


def body(
    random_slabs,
    span_weights,
    wall_filter,
    prev_state,
    time_scale,
    mean_velocity,
    lund_diag,
    lund_off,
):
    rows = random_slabs.shape[0]
    planes = random_slabs.shape[1]
    width = random_slabs.shape[3]
    columns = planes * 3 * width
    half = (span_weights.shape[0] - 1) // 2
    if fits(lax.axis_size("span"), rows, planes, 3, width, half, LANES):
        return exchanged(
            random_slabs,
            span_weights,
            wall_filter,
            prev_state,
            time_scale,
            mean_velocity,
            lund_diag,
            lund_off,
        )
    flat = random_slabs.reshape(rows, columns)
    scaling = jnp.sqrt(jnp.sum(span_weights * span_weights))
    taps = (span_weights / scaling).astype(jnp.bfloat16)
    reach = (span_weights.shape[0] - 1) // 2
    count = lax.axis_size("span")
    slim = columns // count
    held = butterfly(flat.reshape(1, rows, count, slim), True)
    total = rows * count
    whole = held.reshape(total, slim)
    height = min(512, total)
    matrix = band_matrix(taps, height)
    wrapped = jnp.concatenate([whole[total - reach :], whole, whole[:reach]], axis=0)

    def one_block(start):
        window = lax.dynamic_slice_in_dim(wrapped, start, height + 2 * reach, 0)
        return jnp.dot(matrix, window, preferred_element_type=jnp.float32)

    starts = jnp.arange(total // height) * height
    summed_cols = lax.map(one_block, starts).reshape(total, slim)
    rounded = summed_cols.astype(jnp.bfloat16)
    returned = butterfly(rounded.reshape(1, 1, count, rows * slim), False)
    spanned = returned.reshape(count, rows, slim).transpose(1, 0, 2).reshape(rows, planes, 3, width)
    filtered = lax.dot_general(
        spanned, wall_filter, (((3,), (1,)), ((), ())), preferred_element_type=jnp.float32
    )
    decay = jnp.exp(-jnp.pi / (2.0 * time_scale))
    inject = jnp.sqrt(1.0 - jnp.exp(-jnp.pi / time_scale))
    state = prev_state
    outputs = []
    for plane in range(planes):
        state = decay * state + inject * filtered[:, plane]
        along = state[:, 0]
        normal = state[:, 1]
        spanwise = state[:, 2]
        first = mean_velocity + lund_diag[0] * along
        second = lund_off[0] * along + lund_diag[1] * normal
        third = lund_off[1] * along + lund_off[2] * normal + lund_diag[2] * spanwise
        outputs.append(jnp.stack([first, second, third], axis=1).astype(jnp.bfloat16))
    velocity = jnp.stack(outputs, axis=1)
    return (velocity, state)


def solution(mesh):
    placed = (P("span", None, None, None), P(), P(), P("span", None, None), P(), P(), P(), P())
    return jax.shard_map(
        body,
        mesh=mesh,
        in_specs=placed,
        out_specs=(P("span", None, None, None), P("span", None, None)),
        check_vma=False,
    )
```

```python
import functools

import jax
import jax.numpy as jnp
from jax import lax
from jax.experimental import pallas as pl
from jax.experimental.pallas import tpu as pltpu
from jax.sharding import PartitionSpec as P

LANES = 256
GRANT = 44 << 20
MESH = pl.DeviceIdType.MESH


def peer_at(step, me, count, near_first=False):
    half, fourth, chips = count // 2, count // 4, count // 8
    if near_first:
        near, far = step + 1, step - half + 1
        away = step >= half - 1
    else:
        far, near = step // 2, step // 2 + 1
        away = step % 2 == 0
    side = 1 - me // half
    outer = side * 2 + far // fourth
    there = outer * fourth + (me // 2 + far // 2) % chips * 2 + (me + far) % 2
    here = me // half * half + (me + near) % half
    return jnp.where(away, there, here)


def at_distance(away, me, count):
    core, chip = me % 2, me // 2
    layers = count // 8
    layer, aside, along = me // 8, me // 4 % 2, me // 2 % 2
    found = [(me + 1 - 2 * core, None)] if away == 1 else []
    for over in range(1 - layers, layers):
        for turn_aside in range(2):
            for turn_along in range(2):
                if abs(over) + turn_aside + turn_along != away:
                    continue
                other = (
                    chip
                    + over * 4
                    + turn_aside * (2 - 4 * aside)
                    + turn_along * (1 - 2 * along)
                )
                valid = (layer + over >= 0) & (layer + over < layers) if over else None
                found += [(other * 2 + (core + turn) % 2, valid) for turn in range(2)]
    return found


def hops(one, other):
    return (
        jnp.abs(one // 8 - other // 8)
        + jnp.abs(one // 4 % 2 - other // 4 % 2)
        + jnp.abs(one // 2 % 2 - other // 2 % 2)
        + jnp.where(one // 2 == other // 2, 1, 0)
    )


def degree(me, count):
    across = me // 8
    return 5 + 2 * jnp.where(across > 0, 1, 0) + 2 * jnp.where(across < count // 8 - 1, 1, 0)


def visit(away, me, count, run):
    for peer, valid in at_distance(away, me, count):
        if valid is None:
            run(peer)
        else:
            pl.when(valid)(functools.partial(run, peer))


def old_peer_at(step, me, count):
    away = count // 2 + (1 - 2 * (step % 2)) * ((step + 1) // 2)
    return lax.rem(me + away, count)


def exchange_kernel(
    count,
    rows,
    width,
    planes,
    kinds,
    slim,
    reach,
    slab_hbm,
    taps_hbm,
    wall_hbm,
    prev_hbm,
    scale_hbm,
    mean_hbm,
    diag_hbm,
    off_hbm,
    vel_ref,
    state_ref,
    slab,
    taps_ref,
    scale_ref,
    mean_ref,
    diag_ref,
    off_ref,
    x_ref,
    wide,
    summed,
    back,
    band,
    wall,
    turned,
    early_normal,
    early_spanwise,
    along,
    decay,
    inject,
    mixed,
    load_sem,
    slab_sem,
    out_sem,
    in_sem,
    back_out_sem,
    back_in_sem,
    met,
):
    me = lax.axis_index("span")
    blocks = count * rows // reach

    slab_loads = [
        pltpu.make_async_copy(slab_hbm.at[:, kind], slab.at[kind], slab_sem.at[kind])
        for kind in range(kinds)
    ]
    loads = [
        pltpu.make_async_copy(source, target, load_sem.at[at])
        for at, (source, target) in enumerate(
            (
                (taps_hbm, taps_ref),
                (scale_hbm, scale_ref),
                (mean_hbm, mean_ref),
                (diag_hbm, diag_ref),
                (off_hbm, off_ref),
                (prev_hbm, state_ref),
                (wall_hbm, wall),
            )
        )
    ]
    slab_loads[0].start()
    barrier = pltpu.get_barrier_semaphore()

    def greet(semaphore):
        visit(
            1,
            me,
            count,
            lambda peer: pl.semaphore_signal(
                semaphore, inc=1, device_id=(peer,), device_id_type=MESH
            ),
        )

    greet(barrier)
    for load in slab_loads[1:]:
        load.start()
    for load in loads:
        load.start()

    def relayout(kind):
        slab_loads[kind].wait()
        for tile in range(width // 128):
            lanes = slice(tile * 128, (tile + 1) * 128)
            mixed[tile] = slab[kind, :, :, lanes].reshape(rows * planes, 128).astype(jnp.float32)
            for plane in range(planes):
                x_ref[kind, plane, :, lanes] = mixed[tile, pl.ds(plane, rows, planes), :].astype(
                    jnp.bfloat16
                )

    half, chips = count // 2, count // 8

    def columns(owner):
        block = owner // half * chips + owner // 2 % chips
        plane = owner // (2 * chips) % 2 * 2 + owner % 2
        return plane, pl.ds(pl.multiple_of(block * slim, slim), slim)

    def batch(part, sender, receiver):
        late = (receiver // 2 - sender // 2 + chips) % chips
        far = jnp.where(sender // half == receiver // half, 0, 1 + late // (chips // 2))
        return (0, jnp.minimum(far, 1), far)[part]

    def give(part, peer):
        plane, span = columns(peer)
        pltpu.make_async_remote_copy(
            src_ref=x_ref.at[part, plane, :, span],
            dst_ref=wide.at[part, me],
            send_sem=out_sem.at[part],
            recv_sem=in_sem.at[part],
            device_id=(peer,),
            device_id_type=MESH,
        ).start()

    rounds = count // 8
    relayout(0)
    pl.semaphore_wait(barrier, degree(me, count))
    for round in range(rounds):
        greet(met.at[round])
        visit(round + 1, me, count, functools.partial(give, 0))
        if round + 1 < kinds:
            relayout(round + 1)
        if round == 0:
            visit(1, me, count, functools.partial(give, round + 1))
        pl.semaphore_wait(met.at[round], degree(me, count))
    visit(rounds + 1, me, count, functools.partial(give, 0))

    for part in range(1, kinds):

        @pl.loop(0, count - 1)
        def _(step):
            peer = old_peer_at(step, me, count)
            if part == 1:
                pl.when(hops(me, peer) > 1)(functools.partial(give, part, peer))
            else:
                give(part, peer)

    for part in range(kinds):
        plane, span = columns(me)
        pltpu.make_async_copy(
            x_ref.at[part, plane, :, span], wide.at[part, me], in_sem.at[part]
        ).start()

    for load in loads:
        load.wait()
    weights = jnp.concatenate(
        [taps_ref[...], jnp.zeros((3 * reach - taps_ref.shape[0],), jnp.float32)]
    ).reshape(1, 3 * reach)
    taps = weights / jnp.sqrt(jnp.sum(weights * weights))
    tall = jnp.broadcast_to(taps, (16, 3 * reach))
    line = lax.broadcasted_iota(jnp.int32, (16, 3 * reach), 0)
    for bit in range(4):
        tall = jnp.where((line // (1 << bit)) % 2 == 1, pltpu.roll(tall, 1 << bit, 1), tall)

    @pl.loop(0, reach // 16)
    def _(step):
        first = pl.multiple_of(step * 16, 16)
        rolled = pltpu.roll(tall, first, 1)
        band[pl.ds(first, 16), :] = rolled.astype(jnp.bfloat16)

    piece = min(256, width)

    @pl.loop(0, width // piece)
    def _(down):
        @pl.loop(0, width // piece)
        def _(over):
            here = pl.ds(pl.multiple_of(down * piece, piece), piece)
            there = pl.ds(pl.multiple_of(over * piece, piece), piece)
            turned[there, here] = wall[here, there].T

    decay[...] = jnp.exp(-jnp.pi / (2.0 * scale_ref[...]))
    inject[...] = jnp.sqrt(1.0 - jnp.exp(-jnp.pi / scale_ref[...]))

    for part in range(kinds):
        pltpu.make_async_copy(wide.at[part], wide.at[part], in_sem.at[part]).wait()
        share = reach // rows
        for block in range(blocks):
            total = jnp.zeros((reach, slim), jnp.float32)
            for shift in range(3):
                source = (block - 1 + shift) % blocks
                chunk = wide[part, source * share : (source + 1) * share].reshape(reach, slim)
                total += jnp.dot(
                    band[:, shift * reach : (shift + 1) * reach],
                    chunk,
                    preferred_element_type=jnp.float32,
                )
            summed[part, block * share : (block + 1) * share] = total.astype(
                jnp.bfloat16
            ).reshape(share, rows, slim)

        plane, span = columns(me)

        @pl.loop(0, count - 1)
        def _(step):
            peer = peer_at(step, me, count, True) if part == kinds - 1 else old_peer_at(step, me, count)
            arrival = batch(part, me, peer)
            pltpu.make_async_remote_copy(
                src_ref=summed.at[part, peer],
                dst_ref=back.at[part, plane, :, span],
                send_sem=back_out_sem.at[part],
                recv_sem=back_in_sem.at[part, arrival],
                device_id=(peer,),
                device_id_type=MESH,
            ).start()

        pltpu.make_async_copy(
            summed.at[part, me], back.at[part, plane, :, span], back_in_sem.at[part, 0]
        ).start()

    def advance(part, at, filtered):
        one = pl.ds(part, 1)
        state = state_ref[part, :, at]
        states = []
        for plane in range(planes):
            state = decay[one, at] * state + inject[one, at] * filtered[plane]
            states.append(state)
        state_ref[part, :, at] = state
        return states

    def put(part, at, values):
        for tile in range(values[0].shape[1] // 128):
            lanes = slice(tile * 128, (tile + 1) * 128)
            for plane, value in enumerate(values):
                mixed[tile, pl.ds(plane, rows, planes), :] = value[:, lanes]
            here = pl.ds(pl.multiple_of(at.start + tile * 128, 128), 128)
            vel_ref[:, part, :, here] = (
                mixed[tile].astype(jnp.bfloat16).reshape(rows, planes, 128)
            )

    def put_along(at, filtered):
        states = advance(0, at, filtered)
        for plane, state in enumerate(states):
            along[plane, :, at] = state
        put(0, at, [mean_ref[:, at] + diag_ref[0:1, at] * state for state in states])

    def put_normal(at, filtered):
        states = advance(1, at, filtered)
        values = []
        for plane, state in enumerate(states):
            first = along[plane, :, at]
            values.append(off_ref[0:1, at] * first + diag_ref[1:2, at] * state)
            along[plane, :, at] = off_ref[1:2, at] * first + off_ref[2:3, at] * state
        put(1, at, values)

    def base_spanwise(at, filtered):
        for plane, state in enumerate(advance(2, at, filtered)):
            along[plane, :, at] += diag_ref[2:3, at] * state

    def put_spanwise(at, filtered):
        extra = inject[2:3, at] * filtered[0]
        values = [along[0, :, at] + diag_ref[2:3, at] * extra]
        for plane in range(1, planes):
            extra = decay[2:3, at] * extra + inject[2:3, at] * filtered[plane]
            values.append(along[plane, :, at] + diag_ref[2:3, at] * extra)
        state_ref[2, :, at] += extra
        put(2, at, values)

    def arrived(part, arrival, pieces):
        piece = wide.at[part, 0:pieces]
        pltpu.make_async_copy(piece, piece, back_in_sem.at[part, arrival]).wait()

    def filtering(part, tile, chunks, early, finish):
        tile = min(tile, width)

        @pl.loop(0, width // tile)
        def _(step):
            at = pl.ds(pl.multiple_of(step * tile, tile), tile)
            total = None
            for first, size in chunks:
                reading = pl.ds(first, size)
                term = jnp.dot(
                    back[part, :, :, reading].reshape(planes * rows, size),
                    turned[reading, at],
                    preferred_element_type=jnp.float32,
                )
                total = term if total is None else total + term
            total = total.reshape(planes, rows, tile)
            if early is not None:
                total += early[:, :, at]
            finish(at, total)

    def keep(early):
        def run(at, filtered):
            early[:, :, at] = filtered

        return run

    ours = me // half
    near = [(pl.multiple_of(ours * (width // 2), width // 2), width // 2)]
    far = [(pl.multiple_of((1 - ours) * (width // 2), width // 2), width // 2)]
    turns = [(me // 2 - late + chips) % chips for late in range(chips)]
    late = [
        (pl.multiple_of(((1 - ours) * chips + turn) * slim, slim), slim) for turn in turns
    ]
    arrived(0, 0, count)
    filtering(0, 512, [(0, width)], None, put_along)
    arrived(1, 0, half)
    filtering(1, 1024, near, None, keep(early_normal))
    arrived(2, 0, half)
    filtering(2, 1024, near, None, keep(early_spanwise))
    arrived(1, 1, half)
    filtering(1, 1024, far, early_normal, put_normal)
    arrived(2, 1, half // 2)
    filtering(2, 1024, late[: chips // 2], early_spanwise, base_spanwise)
    arrived(2, 2, half // 2)
    filtering(2, 2048, late[chips // 2 :], None, put_spanwise)

    for part in range(kinds):
        sent = wide.at[part, 0 : count - 1]
        pltpu.make_async_copy(sent, sent, out_sem.at[part]).wait()
        pltpu.make_async_copy(sent, sent, back_out_sem.at[part]).wait()


def store_kernel(vel_ref, state_ref, vel_out, state_out, sem):
    copies = (
        pltpu.make_async_copy(vel_ref, vel_out, sem.at[0]),
        pltpu.make_async_copy(state_ref, state_out, sem.at[1]),
    )
    for copy in copies:
        copy.start()
    for copy in copies:
        copy.wait()


def fits(count, rows, planes, kinds, width, reach, slim):
    return (
        planes * width == count * slim
        and kinds == 3
        and planes == 4
        and count % 16 == 0
        and rows % 16 == 0
        and reach % rows == 0
        and reach % 128 == 0
        and count * rows % reach == 0
        and count * rows // reach >= 3
    )


def exchanged(
    random_slabs,
    span_weights,
    wall_filter,
    prev_state,
    time_scale,
    mean_velocity,
    lund_diag,
    lund_off,
):
    count = lax.axis_size("span")
    rows, planes, kinds, width = random_slabs.shape
    reach = (span_weights.shape[0] - 1) // 2
    slim = LANES
    operands = (
        random_slabs.transpose(0, 2, 1, 3),
        span_weights,
        wall_filter,
        prev_state.transpose(1, 0, 2),
        time_scale,
        mean_velocity.reshape(1, width),
        lund_diag,
        lund_off,
    )
    operands = [pltpu.with_memory_space_constraint(each, pltpu.HBM) for each in operands]
    in_vmem = pl.BlockSpec(memory_space=pltpu.VMEM)
    in_hbm = pl.BlockSpec(memory_space=pltpu.HBM)
    fine = (kinds, width)
    velocity, state = pl.pallas_call(
        functools.partial(exchange_kernel, count, rows, width, planes, kinds, slim, reach),
        out_shape=(
            pltpu.VMEM((rows, kinds, planes, width), jnp.bfloat16),
            pltpu.VMEM((kinds, rows, width), jnp.float32),
        ),
        in_specs=[in_hbm] * len(operands),
        out_specs=(in_vmem, in_vmem),
        scratch_shapes=[
            pltpu.VMEM((kinds, rows, planes, width), jnp.bfloat16),
            pltpu.VMEM(span_weights.shape, jnp.float32),
            pltpu.VMEM(fine, jnp.float32),
            pltpu.VMEM((1, width), jnp.float32),
            pltpu.VMEM(fine, jnp.float32),
            pltpu.VMEM(fine, jnp.float32),
            pltpu.VMEM((kinds, planes, rows, width), jnp.bfloat16),
            pltpu.VMEM((kinds, count, rows, slim), jnp.bfloat16),
            pltpu.VMEM((kinds, count, rows, slim), jnp.bfloat16),
            pltpu.VMEM((kinds, planes, rows, width), jnp.bfloat16),
            pltpu.VMEM((reach, 3 * reach), jnp.bfloat16),
            pltpu.VMEM((width, width), jnp.bfloat16),
            pltpu.VMEM((width, width), jnp.bfloat16),
            pltpu.VMEM((planes, rows, width), jnp.float32),
            pltpu.VMEM((planes, rows, width), jnp.float32),
            pltpu.VMEM((planes, rows, width), jnp.float32),
            pltpu.VMEM(fine, jnp.float32),
            pltpu.VMEM(fine, jnp.float32),
            pltpu.VMEM((width // 128, rows * planes, 128), jnp.float32),
            pltpu.SemaphoreType.DMA((7,)),
            pltpu.SemaphoreType.DMA((kinds,)),
            pltpu.SemaphoreType.DMA((kinds,)),
            pltpu.SemaphoreType.DMA((kinds,)),
            pltpu.SemaphoreType.DMA((kinds,)),
            pltpu.SemaphoreType.DMA((kinds, 3)),
            pltpu.SemaphoreType.REGULAR((count // 8,)),
        ],
        compiler_params=pltpu.CompilerParams(
            collective_id=0, has_side_effects=True, vmem_limit_bytes=GRANT
        ),
    )(*operands)
    velocity, state = pl.pallas_call(
        store_kernel,
        out_shape=(
            jax.ShapeDtypeStruct(velocity.shape, velocity.dtype),
            jax.ShapeDtypeStruct(state.shape, state.dtype),
        ),
        in_specs=[in_vmem, in_vmem],
        out_specs=(in_hbm, in_hbm),
        scratch_shapes=[pltpu.SemaphoreType.DMA((2,))],
        compiler_params=pltpu.CompilerParams(vmem_limit_bytes=GRANT),
    )(velocity, state)
    return velocity.transpose(0, 2, 1, 3), state.transpose(1, 0, 2)


def from_partner(value, axis, bit):
    return lax.ppermute(value, axis, [(i, i ^ 1 << bit) for i in range(lax.axis_size(axis))])


def band_matrix(taps, height):
    reach = taps.shape[0]
    padded = jnp.concatenate([taps, jnp.zeros((height,), taps.dtype)])
    length = reach + height
    tiled = jnp.tile(padded, height)[: height * (length - 1)]
    return tiled.reshape(height, length - 1)


def butterfly(held, forward):
    count = lax.axis_size("span")
    device = lax.axis_index("span")
    levels = count.bit_length() - 1
    for level in range(levels - 1, -1, -1):
        groups, inner_first, targets, inner_last = held.shape
        halves = held.reshape(groups, inner_first, 2, targets // 2, inner_last)
        lower = halves[:, :, 0]
        higher = halves[:, :, 1]
        upper = device >> level & 1 == 1
        kept = jnp.where(upper, higher, lower)
        given = jnp.where(upper, lower, higher)
        if forward:
            taken = from_partner(given, "span", level)
        else:
            taken = from_partner(given, "span", level)
        first = jnp.where(upper, taken, kept)
        second = jnp.where(upper, kept, taken)
        held = jnp.stack([first, second], axis=1).reshape(
            groups * 2, inner_first, targets // 2, inner_last
        )
    return held


def body(
    random_slabs,
    span_weights,
    wall_filter,
    prev_state,
    time_scale,
    mean_velocity,
    lund_diag,
    lund_off,
):
    rows = random_slabs.shape[0]
    planes = random_slabs.shape[1]
    width = random_slabs.shape[3]
    columns = planes * 3 * width
    half = (span_weights.shape[0] - 1) // 2
    if fits(lax.axis_size("span"), rows, planes, 3, width, half, LANES):
        return exchanged(
            random_slabs,
            span_weights,
            wall_filter,
            prev_state,
            time_scale,
            mean_velocity,
            lund_diag,
            lund_off,
        )
    flat = random_slabs.reshape(rows, columns)
    scaling = jnp.sqrt(jnp.sum(span_weights * span_weights))
    taps = (span_weights / scaling).astype(jnp.bfloat16)
    reach = (span_weights.shape[0] - 1) // 2
    count = lax.axis_size("span")
    slim = columns // count
    held = butterfly(flat.reshape(1, rows, count, slim), True)
    total = rows * count
    whole = held.reshape(total, slim)
    height = min(512, total)
    matrix = band_matrix(taps, height)
    wrapped = jnp.concatenate([whole[total - reach :], whole, whole[:reach]], axis=0)

    def one_block(start):
        window = lax.dynamic_slice_in_dim(wrapped, start, height + 2 * reach, 0)
        return jnp.dot(matrix, window, preferred_element_type=jnp.float32)

    starts = jnp.arange(total // height) * height
    summed_cols = lax.map(one_block, starts).reshape(total, slim)
    rounded = summed_cols.astype(jnp.bfloat16)
    returned = butterfly(rounded.reshape(1, 1, count, rows * slim), False)
    spanned = returned.reshape(count, rows, slim).transpose(1, 0, 2).reshape(rows, planes, 3, width)
    filtered = lax.dot_general(
        spanned, wall_filter, (((3,), (1,)), ((), ())), preferred_element_type=jnp.float32
    )
    decay = jnp.exp(-jnp.pi / (2.0 * time_scale))
    inject = jnp.sqrt(1.0 - jnp.exp(-jnp.pi / time_scale))
    state = prev_state
    outputs = []
    for plane in range(planes):
        state = decay * state + inject * filtered[:, plane]
        along = state[:, 0]
        normal = state[:, 1]
        spanwise = state[:, 2]
        first = mean_velocity + lund_diag[0] * along
        second = lund_off[0] * along + lund_diag[1] * normal
        third = lund_off[1] * along + lund_off[2] * normal + lund_diag[2] * spanwise
        outputs.append(jnp.stack([first, second, third], axis=1).astype(jnp.bfloat16))
    velocity = jnp.stack(outputs, axis=1)
    return (velocity, state)


def solution(mesh):
    placed = (P("span", None, None, None), P(), P(), P("span", None, None), P(), P(), P(), P())
    return jax.shard_map(
        body,
        mesh=mesh,
        in_specs=placed,
        out_specs=(P("span", None, None, None), P("span", None, None)),
        check_vma=False,
    )
```

```python
import functools

import jax
import jax.numpy as jnp
from jax import lax
from jax.experimental import pallas as pl
from jax.experimental.pallas import tpu as pltpu
from jax.sharding import PartitionSpec as P

LANES = 256
GRANT = 44 << 20
CUTS = 2
MESH = pl.DeviceIdType.MESH


def peer_at(step, me, count, near_first=False):
    half, fourth, chips = count // 2, count // 4, count // 8
    if near_first:
        near, far = step + 1, step - half + 1
        away = step >= half - 1
    else:
        far, near = step // 2, step // 2 + 1
        away = step % 2 == 0
    side = 1 - me // half
    outer = side * 2 + far // fourth
    there = outer * fourth + (me // 2 + far // 2) % chips * 2 + (me + far) % 2
    here = me // half * half + (me + near) % half
    return jnp.where(away, there, here)


def at_distance(away, me, count):
    core, chip = me % 2, me // 2
    layers = count // 8
    layer, aside, along = me // 8, me // 4 % 2, me // 2 % 2
    found = [(me + 1 - 2 * core, None)] if away == 1 else []
    for over in range(1 - layers, layers):
        for turn_aside in range(2):
            for turn_along in range(2):
                if abs(over) + turn_aside + turn_along != away:
                    continue
                other = (
                    chip
                    + over * 4
                    + turn_aside * (2 - 4 * aside)
                    + turn_along * (1 - 2 * along)
                )
                valid = (layer + over >= 0) & (layer + over < layers) if over else None
                found += [(other * 2 + (core + turn) % 2, valid) for turn in range(2)]
    return found


def hops(one, other):
    return (
        jnp.abs(one // 8 - other // 8)
        + jnp.abs(one // 4 % 2 - other // 4 % 2)
        + jnp.abs(one // 2 % 2 - other // 2 % 2)
        + jnp.where(one // 2 == other // 2, 1, 0)
    )


def degree(me, count):
    across = me // 8
    return 5 + 2 * jnp.where(across > 0, 1, 0) + 2 * jnp.where(across < count // 8 - 1, 1, 0)


def visit(away, me, count, run):
    for peer, valid in at_distance(away, me, count):
        if valid is None:
            run(peer)
        else:
            pl.when(valid)(functools.partial(run, peer))


def old_peer_at(step, me, count):
    away = count // 2 + (1 - 2 * (step % 2)) * ((step + 1) // 2)
    return lax.rem(me + away, count)


def weave(target, mixed, at, values):
    planes, rows = len(values), values[0].shape[0]
    for tile in range(values[0].shape[1] // 128):
        lanes = slice(tile * 128, (tile + 1) * 128)
        for plane, value in enumerate(values):
            mixed[tile, pl.ds(plane, rows, planes), :] = value[:, lanes]
        here = pl.ds(pl.multiple_of(at.start + tile * 128, 128), 128)
        target[:, :, here] = mixed[tile].astype(jnp.bfloat16).reshape(rows, planes, 128)


def exchange_kernel(
    count,
    rows,
    width,
    planes,
    kinds,
    slim,
    reach,
    slab_hbm,
    taps_hbm,
    wall_hbm,
    prev_hbm,
    scale_hbm,
    mean_hbm,
    diag_hbm,
    off_hbm,
    vel_ref,
    state_ref,
    along,
    tail_ref,
    tail_wall_ref,
    tail_factors_ref,
    slab,
    taps_ref,
    scale_ref,
    mean_ref,
    diag_ref,
    off_ref,
    x_ref,
    wide,
    summed,
    back,
    band,
    wall,
    turned,
    early_normal,
    early_spanwise,
    decay,
    inject,
    mixed,
    load_sem,
    slab_sem,
    out_sem,
    in_sem,
    back_out_sem,
    back_in_sem,
    met,
):
    me = lax.axis_index("span")
    blocks = count * rows // reach

    slab_loads = [
        pltpu.make_async_copy(slab_hbm.at[:, kind], slab.at[kind], slab_sem.at[kind])
        for kind in range(kinds)
    ]
    loads = [
        pltpu.make_async_copy(source, target, load_sem.at[at])
        for at, (source, target) in enumerate(
            (
                (taps_hbm, taps_ref),
                (scale_hbm, scale_ref),
                (mean_hbm, mean_ref),
                (diag_hbm, diag_ref),
                (off_hbm, off_ref),
                (prev_hbm, state_ref),
                (wall_hbm, wall),
            )
        )
    ]
    slab_loads[0].start()
    barrier = pltpu.get_barrier_semaphore()

    def greet(semaphore):
        visit(
            1,
            me,
            count,
            lambda peer: pl.semaphore_signal(
                semaphore, inc=1, device_id=(peer,), device_id_type=MESH
            ),
        )

    greet(barrier)
    for load in slab_loads[1:]:
        load.start()
    for load in loads:
        load.start()

    def relayout(kind):
        slab_loads[kind].wait()
        for tile in range(width // 128):
            lanes = slice(tile * 128, (tile + 1) * 128)
            mixed[tile] = slab[kind, :, :, lanes].reshape(rows * planes, 128).astype(jnp.float32)
            for plane in range(planes):
                x_ref[kind, plane, :, lanes] = mixed[tile, pl.ds(plane, rows, planes), :].astype(
                    jnp.bfloat16
                )

    half, chips = count // 2, count // 8

    def columns(owner):
        block = owner // half * chips + owner // 2 % chips
        plane = owner // (2 * chips) % 2 * 2 + owner % 2
        return plane, pl.ds(pl.multiple_of(block * slim, slim), slim)

    def batch(part, sender, receiver):
        late = (receiver // 2 - sender // 2 + chips) % chips
        far = jnp.where(sender // half == receiver // half, 0, 1 + late // (chips // 2))
        return (0, jnp.minimum(far, 1), far)[part]

    def give(part, peer):
        plane, span = columns(peer)
        pltpu.make_async_remote_copy(
            src_ref=x_ref.at[part, plane, :, span],
            dst_ref=wide.at[part, me],
            send_sem=out_sem.at[part],
            recv_sem=in_sem.at[part],
            device_id=(peer,),
            device_id_type=MESH,
        ).start()

    rounds = count // 8
    relayout(0)
    pl.semaphore_wait(barrier, degree(me, count))
    for round in range(rounds):
        greet(met.at[round])
        visit(round + 1, me, count, functools.partial(give, 0))
        if round + 1 < kinds:
            relayout(round + 1)
        if round == 0:
            visit(1, me, count, functools.partial(give, round + 1))
        pl.semaphore_wait(met.at[round], degree(me, count))
    visit(rounds + 1, me, count, functools.partial(give, 0))

    for part in range(1, kinds):

        @pl.loop(0, count - 1)
        def _(step):
            peer = old_peer_at(step, me, count)
            if part == 1:
                pl.when(hops(me, peer) > 1)(functools.partial(give, part, peer))
            else:
                give(part, peer)

    for part in range(kinds):
        plane, span = columns(me)
        pltpu.make_async_copy(
            x_ref.at[part, plane, :, span], wide.at[part, me], in_sem.at[part]
        ).start()

    for load in loads:
        load.wait()
    weights = jnp.concatenate(
        [taps_ref[...], jnp.zeros((3 * reach - taps_ref.shape[0],), jnp.float32)]
    ).reshape(1, 3 * reach)
    taps = weights / jnp.sqrt(jnp.sum(weights * weights))
    tall = jnp.broadcast_to(taps, (16, 3 * reach))
    line = lax.broadcasted_iota(jnp.int32, (16, 3 * reach), 0)
    for bit in range(4):
        tall = jnp.where((line // (1 << bit)) % 2 == 1, pltpu.roll(tall, 1 << bit, 1), tall)

    @pl.loop(0, reach // 16)
    def _(step):
        first = pl.multiple_of(step * 16, 16)
        rolled = pltpu.roll(tall, first, 1)
        band[pl.ds(first, 16), :] = rolled.astype(jnp.bfloat16)

    piece = min(256, width)

    @pl.loop(0, width // piece)
    def _(down):
        @pl.loop(0, width // piece)
        def _(over):
            here = pl.ds(pl.multiple_of(down * piece, piece), piece)
            there = pl.ds(pl.multiple_of(over * piece, piece), piece)
            turned[there, here] = wall[here, there].T

    decay[...] = jnp.exp(-jnp.pi / (2.0 * scale_ref[...]))
    inject[...] = jnp.sqrt(1.0 - jnp.exp(-jnp.pi / scale_ref[...]))

    for part in range(kinds):
        pltpu.make_async_copy(wide.at[part], wide.at[part], in_sem.at[part]).wait()
        share = reach // rows
        for block in range(blocks):
            total = jnp.zeros((reach, slim), jnp.float32)
            for shift in range(3):
                source = (block - 1 + shift) % blocks
                chunk = wide[part, source * share : (source + 1) * share].reshape(reach, slim)
                total += jnp.dot(
                    band[:, shift * reach : (shift + 1) * reach],
                    chunk,
                    preferred_element_type=jnp.float32,
                )
            summed[part, block * share : (block + 1) * share] = total.astype(
                jnp.bfloat16
            ).reshape(share, rows, slim)

        plane, span = columns(me)

        @pl.loop(0, count - 1)
        def _(step):
            peer = peer_at(step, me, count, True) if part == kinds - 1 else old_peer_at(step, me, count)
            arrival = batch(part, me, peer)
            pltpu.make_async_remote_copy(
                src_ref=summed.at[part, peer],
                dst_ref=back.at[part, plane, :, span],
                send_sem=back_out_sem.at[part],
                recv_sem=back_in_sem.at[part, arrival],
                device_id=(peer,),
                device_id_type=MESH,
            ).start()

        pltpu.make_async_copy(
            summed.at[part, me], back.at[part, plane, :, span], back_in_sem.at[part, 0]
        ).start()

    def advance(part, at, filtered):
        one = pl.ds(part, 1)
        state = state_ref[part, :, at]
        states = []
        for plane in range(planes):
            state = decay[one, at] * state + inject[one, at] * filtered[plane]
            states.append(state)
        state_ref[part, :, at] = state
        return states

    def put_along(at, filtered):
        states = advance(0, at, filtered)
        for plane, state in enumerate(states):
            along[plane, :, at] = state
        weave(vel_ref.at[:, 0], mixed, at, [mean_ref[:, at] + diag_ref[0:1, at] * state for state in states])

    def put_normal(at, filtered):
        states = advance(1, at, filtered)
        values = []
        for plane, state in enumerate(states):
            first = along[plane, :, at]
            values.append(off_ref[0:1, at] * first + diag_ref[1:2, at] * state)
            along[plane, :, at] = off_ref[1:2, at] * first + off_ref[2:3, at] * state
        weave(vel_ref.at[:, 1], mixed, at, values)

    def base_spanwise(at, filtered):
        for plane, state in enumerate(advance(2, at, filtered)):
            along[plane, :, at] += diag_ref[2:3, at] * state

    def arrived(part, arrival, pieces):
        piece = wide.at[part, 0:pieces]
        pltpu.make_async_copy(piece, piece, back_in_sem.at[part, arrival]).wait()

    def filtering(part, tile, chunks, early, finish):
        tile = min(tile, width)

        @pl.loop(0, width // tile)
        def _(step):
            at = pl.ds(pl.multiple_of(step * tile, tile), tile)
            total = None
            for first, size in chunks:
                reading = pl.ds(first, size)
                term = jnp.dot(
                    back[part, :, :, reading].reshape(planes * rows, size),
                    turned[reading, at],
                    preferred_element_type=jnp.float32,
                )
                total = term if total is None else total + term
            total = total.reshape(planes, rows, tile)
            if early is not None:
                total += early[:, :, at]
            finish(at, total)

    def keep(early):
        def run(at, filtered):
            early[:, :, at] = filtered

        return run

    ours = me // half
    near = [(pl.multiple_of(ours * (width // 2), width // 2), width // 2)]
    far = [(pl.multiple_of((1 - ours) * (width // 2), width // 2), width // 2)]
    turns = [(me // 2 - late + chips) % chips for late in range(chips)]
    late = [
        (pl.multiple_of(((1 - ours) * chips + turn) * slim, slim), slim) for turn in turns
    ]
    for at, (first, size) in enumerate(late[chips // 2 :]):
        tail_wall_ref[at * slim : (at + 1) * slim] = turned[pl.ds(first, size)]
    for at, source in enumerate((decay, inject, diag_ref)):
        tail_factors_ref[at : at + 1] = source[2:3]
    arrived(0, 0, count)
    filtering(0, 512, [(0, width)], None, put_along)
    arrived(1, 0, half)
    filtering(1, 1024, near, None, keep(early_normal))
    arrived(2, 0, half)
    filtering(2, 1024, near, None, keep(early_spanwise))
    arrived(1, 1, half)
    filtering(1, 1024, far, early_normal, put_normal)
    arrived(2, 1, half // 2)
    filtering(2, 1024, late[: chips // 2], early_spanwise, base_spanwise)
    arrived(2, 2, half // 2)
    for at, (first, size) in enumerate(late[chips // 2 :]):
        tail_ref[:, at * slim : (at + 1) * slim] = back[2, :, :, pl.ds(first, size)].reshape(
            planes * rows, size
        )

    for part in range(kinds):
        sent = wide.at[part, 0 : count - 1]
        pltpu.make_async_copy(sent, sent, out_sem.at[part]).wait()
        pltpu.make_async_copy(sent, sent, back_out_sem.at[part]).wait()


def store_kernel(
    vel_ref,
    state_ref,
    base_ref,
    tail_ref,
    wall_ref,
    factors_ref,
    vel_out,
    state_out,
    last,
    last_state,
    mixed,
    sem,
):
    planes, rows, width = base_ref.shape
    kinds = state_ref.shape[0]
    ready = pl.ds(0, kinds - 1)
    copies = [
        pltpu.make_async_copy(vel_ref, vel_out.at[:, ready], sem.at[0]),
        pltpu.make_async_copy(state_ref.at[ready], state_out.at[ready], sem.at[1]),
    ]
    for copy in copies:
        copy.start()
    tile = width // CUTS
    for cut in range(CUTS):
        at = pl.ds(cut * tile, tile)
        filtered = jnp.dot(
            tail_ref[...], wall_ref[:, at], preferred_element_type=jnp.float32
        ).reshape(planes, rows, tile)
        decay, inject, diag = (factors_ref[one : one + 1, at] for one in range(3))
        extra = inject * filtered[0]
        values = [base_ref[0, :, at] + diag * extra]
        for plane in range(1, planes):
            extra = decay * extra + inject * filtered[plane]
            values.append(base_ref[plane, :, at] + diag * extra)
        last_state[:, at] = state_ref[kinds - 1, :, at] + extra
        weave(last, mixed, at, values)
        copies += [
            pltpu.make_async_copy(
                last.at[:, :, at], vel_out.at[:, kinds - 1, :, at], sem.at[2 + 2 * cut]
            ),
            pltpu.make_async_copy(
                last_state.at[:, at], state_out.at[kinds - 1, :, at], sem.at[3 + 2 * cut]
            ),
        ]
        for copy in copies[-2:]:
            copy.start()
    for copy in copies:
        copy.wait()


def fits(count, rows, planes, kinds, width, reach, slim):
    return (
        planes * width == count * slim
        and kinds == 3
        and planes == 4
        and count % 16 == 0
        and rows % 16 == 0
        and reach % rows == 0
        and reach % 128 == 0
        and count * rows % reach == 0
        and count * rows // reach >= 3
    )


def exchanged(
    random_slabs,
    span_weights,
    wall_filter,
    prev_state,
    time_scale,
    mean_velocity,
    lund_diag,
    lund_off,
):
    count = lax.axis_size("span")
    rows, planes, kinds, width = random_slabs.shape
    reach = (span_weights.shape[0] - 1) // 2
    slim = LANES
    operands = (
        random_slabs.transpose(0, 2, 1, 3),
        span_weights,
        wall_filter,
        prev_state.transpose(1, 0, 2),
        time_scale,
        mean_velocity.reshape(1, width),
        lund_diag,
        lund_off,
    )
    operands = [pltpu.with_memory_space_constraint(each, pltpu.HBM) for each in operands]
    in_vmem = pl.BlockSpec(memory_space=pltpu.VMEM)
    in_hbm = pl.BlockSpec(memory_space=pltpu.HBM)
    fine = (kinds, width)
    held = pl.pallas_call(
        functools.partial(exchange_kernel, count, rows, width, planes, kinds, slim, reach),
        out_shape=(
            pltpu.VMEM((rows, kinds - 1, planes, width), jnp.bfloat16),
            pltpu.VMEM((kinds, rows, width), jnp.float32),
            pltpu.VMEM((planes, rows, width), jnp.float32),
            pltpu.VMEM((planes * rows, width // 4), jnp.bfloat16),
            pltpu.VMEM((width // 4, width), jnp.bfloat16),
            pltpu.VMEM(fine, jnp.float32),
        ),
        in_specs=[in_hbm] * len(operands),
        out_specs=(in_vmem,) * 6,
        scratch_shapes=[
            pltpu.VMEM((kinds, rows, planes, width), jnp.bfloat16),
            pltpu.VMEM(span_weights.shape, jnp.float32),
            pltpu.VMEM(fine, jnp.float32),
            pltpu.VMEM((1, width), jnp.float32),
            pltpu.VMEM(fine, jnp.float32),
            pltpu.VMEM(fine, jnp.float32),
            pltpu.VMEM((kinds, planes, rows, width), jnp.bfloat16),
            pltpu.VMEM((kinds, count, rows, slim), jnp.bfloat16),
            pltpu.VMEM((kinds, count, rows, slim), jnp.bfloat16),
            pltpu.VMEM((kinds, planes, rows, width), jnp.bfloat16),
            pltpu.VMEM((reach, 3 * reach), jnp.bfloat16),
            pltpu.VMEM((width, width), jnp.bfloat16),
            pltpu.VMEM((width, width), jnp.bfloat16),
            pltpu.VMEM((planes, rows, width), jnp.float32),
            pltpu.VMEM((planes, rows, width), jnp.float32),
            pltpu.VMEM(fine, jnp.float32),
            pltpu.VMEM(fine, jnp.float32),
            pltpu.VMEM((width // 128, rows * planes, 128), jnp.float32),
            pltpu.SemaphoreType.DMA((7,)),
            pltpu.SemaphoreType.DMA((kinds,)),
            pltpu.SemaphoreType.DMA((kinds,)),
            pltpu.SemaphoreType.DMA((kinds,)),
            pltpu.SemaphoreType.DMA((kinds,)),
            pltpu.SemaphoreType.DMA((kinds, 3)),
            pltpu.SemaphoreType.REGULAR((count // 8,)),
        ],
        compiler_params=pltpu.CompilerParams(
            collective_id=0, has_side_effects=True, vmem_limit_bytes=GRANT
        ),
    )(*operands)
    velocity, state = pl.pallas_call(
        store_kernel,
        out_shape=(
            jax.ShapeDtypeStruct((rows, kinds, planes, width), jnp.bfloat16),
            jax.ShapeDtypeStruct((kinds, rows, width), jnp.float32),
        ),
        in_specs=[in_vmem] * len(held),
        out_specs=(in_hbm, in_hbm),
        scratch_shapes=[
            pltpu.VMEM((rows, planes, width), jnp.bfloat16),
            pltpu.VMEM((rows, width), jnp.float32),
            pltpu.VMEM((width // 128, rows * planes, 128), jnp.float32),
            pltpu.SemaphoreType.DMA((2 + 2 * CUTS,)),
        ],
        compiler_params=pltpu.CompilerParams(vmem_limit_bytes=GRANT // 2),
    )(*held)
    return velocity.transpose(0, 2, 1, 3), state.transpose(1, 0, 2)


def from_partner(value, axis, bit):
    return lax.ppermute(value, axis, [(i, i ^ 1 << bit) for i in range(lax.axis_size(axis))])


def band_matrix(taps, height):
    reach = taps.shape[0]
    padded = jnp.concatenate([taps, jnp.zeros((height,), taps.dtype)])
    length = reach + height
    tiled = jnp.tile(padded, height)[: height * (length - 1)]
    return tiled.reshape(height, length - 1)


def butterfly(held, forward):
    count = lax.axis_size("span")
    device = lax.axis_index("span")
    levels = count.bit_length() - 1
    for level in range(levels - 1, -1, -1):
        groups, inner_first, targets, inner_last = held.shape
        halves = held.reshape(groups, inner_first, 2, targets // 2, inner_last)
        lower = halves[:, :, 0]
        higher = halves[:, :, 1]
        upper = device >> level & 1 == 1
        kept = jnp.where(upper, higher, lower)
        given = jnp.where(upper, lower, higher)
        if forward:
            taken = from_partner(given, "span", level)
        else:
            taken = from_partner(given, "span", level)
        first = jnp.where(upper, taken, kept)
        second = jnp.where(upper, kept, taken)
        held = jnp.stack([first, second], axis=1).reshape(
            groups * 2, inner_first, targets // 2, inner_last
        )
    return held


def body(
    random_slabs,
    span_weights,
    wall_filter,
    prev_state,
    time_scale,
    mean_velocity,
    lund_diag,
    lund_off,
):
    rows = random_slabs.shape[0]
    planes = random_slabs.shape[1]
    width = random_slabs.shape[3]
    columns = planes * 3 * width
    half = (span_weights.shape[0] - 1) // 2
    if fits(lax.axis_size("span"), rows, planes, 3, width, half, LANES):
        return exchanged(
            random_slabs,
            span_weights,
            wall_filter,
            prev_state,
            time_scale,
            mean_velocity,
            lund_diag,
            lund_off,
        )
    flat = random_slabs.reshape(rows, columns)
    scaling = jnp.sqrt(jnp.sum(span_weights * span_weights))
    taps = (span_weights / scaling).astype(jnp.bfloat16)
    reach = (span_weights.shape[0] - 1) // 2
    count = lax.axis_size("span")
    slim = columns // count
    held = butterfly(flat.reshape(1, rows, count, slim), True)
    total = rows * count
    whole = held.reshape(total, slim)
    height = min(512, total)
    matrix = band_matrix(taps, height)
    wrapped = jnp.concatenate([whole[total - reach :], whole, whole[:reach]], axis=0)

    def one_block(start):
        window = lax.dynamic_slice_in_dim(wrapped, start, height + 2 * reach, 0)
        return jnp.dot(matrix, window, preferred_element_type=jnp.float32)

    starts = jnp.arange(total // height) * height
    summed_cols = lax.map(one_block, starts).reshape(total, slim)
    rounded = summed_cols.astype(jnp.bfloat16)
    returned = butterfly(rounded.reshape(1, 1, count, rows * slim), False)
    spanned = returned.reshape(count, rows, slim).transpose(1, 0, 2).reshape(rows, planes, 3, width)
    filtered = lax.dot_general(
        spanned, wall_filter, (((3,), (1,)), ((), ())), preferred_element_type=jnp.float32
    )
    decay = jnp.exp(-jnp.pi / (2.0 * time_scale))
    inject = jnp.sqrt(1.0 - jnp.exp(-jnp.pi / time_scale))
    state = prev_state
    outputs = []
    for plane in range(planes):
        state = decay * state + inject * filtered[:, plane]
        along = state[:, 0]
        normal = state[:, 1]
        spanwise = state[:, 2]
        first = mean_velocity + lund_diag[0] * along
        second = lund_off[0] * along + lund_diag[1] * normal
        third = lund_off[1] * along + lund_off[2] * normal + lund_diag[2] * spanwise
        outputs.append(jnp.stack([first, second, third], axis=1).astype(jnp.bfloat16))
    velocity = jnp.stack(outputs, axis=1)
    return (velocity, state)


def solution(mesh):
    placed = (P("span", None, None, None), P(), P(), P("span", None, None), P(), P(), P(), P())
    return jax.shard_map(
        body,
        mesh=mesh,
        in_specs=placed,
        out_specs=(P("span", None, None, None), P("span", None, None)),
        check_vma=False,
    )
```

```python
import functools

import jax
import jax.numpy as jnp
from jax import lax
from jax.experimental import pallas as pl
from jax.experimental.pallas import tpu as pltpu
from jax.sharding import PartitionSpec as P

LANES = 256
GRANT = 44 << 20
CUTS = 2
MESH = pl.DeviceIdType.MESH


def peer_at(step, me, count, near_first=False):
    half, fourth, chips = count // 2, count // 4, count // 8
    if near_first:
        near, far = step + 1, step - half + 1
        away = step >= half - 1
    else:
        far, near = step // 2, step // 2 + 1
        away = step % 2 == 0
    side = 1 - me // half
    outer = side * 2 + far // fourth
    there = outer * fourth + (me // 2 + far // 2) % chips * 2 + (me + far) % 2
    here = me // half * half + (me + near) % half
    return jnp.where(away, there, here)


def at_distance(away, me, count):
    core, chip = me % 2, me // 2
    layers = count // 8
    layer, aside, along = me // 8, me // 4 % 2, me // 2 % 2
    found = [(me + 1 - 2 * core, None)] if away == 1 else []
    for over in range(1 - layers, layers):
        for turn_aside in range(2):
            for turn_along in range(2):
                if abs(over) + turn_aside + turn_along != away:
                    continue
                other = (
                    chip
                    + over * 4
                    + turn_aside * (2 - 4 * aside)
                    + turn_along * (1 - 2 * along)
                )
                valid = (layer + over >= 0) & (layer + over < layers) if over else None
                found += [(other * 2 + (core + turn) % 2, valid) for turn in range(2)]
    return found


def hops(one, other):
    return (
        jnp.abs(one // 8 - other // 8)
        + jnp.abs(one // 4 % 2 - other // 4 % 2)
        + jnp.abs(one // 2 % 2 - other // 2 % 2)
        + jnp.where(one // 2 == other // 2, 1, 0)
    )


def degree(me, count):
    across = me // 8
    return 5 + 2 * jnp.where(across > 0, 1, 0) + 2 * jnp.where(across < count // 8 - 1, 1, 0)


def visit(away, me, count, run):
    for peer, valid in at_distance(away, me, count):
        if valid is None:
            run(peer)
        else:
            pl.when(valid)(functools.partial(run, peer))


def old_peer_at(step, me, count):
    away = count // 2 + (1 - 2 * (step % 2)) * ((step + 1) // 2)
    return lax.rem(me + away, count)


def weave(target, mixed, at, values):
    planes, rows = len(values), values[0].shape[0]
    for tile in range(values[0].shape[1] // 128):
        lanes = slice(tile * 128, (tile + 1) * 128)
        for plane, value in enumerate(values):
            mixed[tile, pl.ds(plane, rows, planes), :] = value[:, lanes]
        here = pl.ds(pl.multiple_of(at.start + tile * 128, 128), 128)
        target[:, :, here] = mixed[tile].astype(jnp.bfloat16).reshape(rows, planes, 128)


def exchange_kernel(
    count,
    rows,
    width,
    planes,
    kinds,
    slim,
    reach,
    slab_hbm,
    taps_hbm,
    wall_hbm,
    prev_hbm,
    scale_hbm,
    mean_hbm,
    diag_hbm,
    off_hbm,
    vel_ref,
    state_ref,
    along,
    tail_ref,
    tail_wall_ref,
    tail_factors_ref,
    slab,
    taps_ref,
    scale_ref,
    mean_ref,
    diag_ref,
    off_ref,
    x_ref,
    wide,
    summed,
    back,
    band,
    wall,
    turned,
    early_normal,
    early_spanwise,
    decay,
    inject,
    mixed,
    load_sem,
    slab_sem,
    out_sem,
    in_sem,
    back_out_sem,
    back_in_sem,
    met,
):
    me = lax.axis_index("span")
    blocks = count * rows // reach

    slab_loads = [
        pltpu.make_async_copy(slab_hbm.at[:, kind], slab.at[kind], slab_sem.at[kind])
        for kind in range(kinds)
    ]
    loads = [
        pltpu.make_async_copy(source, target, load_sem.at[at])
        for at, (source, target) in enumerate(
            (
                (taps_hbm, taps_ref),
                (scale_hbm, scale_ref),
                (mean_hbm, mean_ref),
                (diag_hbm, diag_ref),
                (off_hbm, off_ref),
                (prev_hbm, state_ref),
                (wall_hbm, wall),
            )
        )
    ]
    slab_loads[0].start()
    barrier = pltpu.get_barrier_semaphore()

    def greet(semaphore):
        visit(
            1,
            me,
            count,
            lambda peer: pl.semaphore_signal(
                semaphore, inc=1, device_id=(peer,), device_id_type=MESH
            ),
        )

    greet(barrier)
    for load in slab_loads[1:]:
        load.start()
    for load in loads:
        load.start()

    def relayout(kind):
        slab_loads[kind].wait()
        for tile in range(width // 128):
            lanes = slice(tile * 128, (tile + 1) * 128)
            block_lanes = slice(tile * 128 % slim, tile * 128 % slim + 128)
            mixed[tile] = slab[kind, :, :, lanes].reshape(rows * planes, 128).astype(jnp.float32)
            for plane in range(planes):
                x_ref[kind, plane, tile * 128 // slim, :, block_lanes] = mixed[tile, pl.ds(plane, rows, planes), :].astype(
                    jnp.bfloat16
                )

    half, chips = count // 2, count // 8

    def columns(owner):
        block = owner // half * chips + owner // 2 % chips
        plane = owner // (2 * chips) % 2 * 2 + owner % 2
        return plane, block

    def batch(part, sender, receiver):
        late = (receiver // 2 - sender // 2 + chips) % chips
        far = jnp.where(sender // half == receiver // half, 0, 1 + jnp.minimum(late, 1))
        return (0, jnp.minimum(far, 1), far)[part]

    def give(part, peer):
        plane, span = columns(peer)
        pltpu.make_async_remote_copy(
            src_ref=x_ref.at[part, plane, span],
            dst_ref=wide.at[part, me],
            send_sem=out_sem.at[part],
            recv_sem=in_sem.at[part],
            device_id=(peer,),
            device_id_type=MESH,
        ).start()

    rounds = count // 8
    relayout(0)
    pl.semaphore_wait(barrier, degree(me, count))
    for round in range(rounds):
        greet(met.at[round])
        visit(round + 1, me, count, functools.partial(give, 0))
        if round + 1 < kinds:
            relayout(round + 1)
        if round == 0:
            visit(1, me, count, functools.partial(give, round + 1))
        pl.semaphore_wait(met.at[round], degree(me, count))
    visit(rounds + 1, me, count, functools.partial(give, 0))

    for part in range(1, kinds):

        @pl.loop(0, count - 1)
        def _(step):
            peer = old_peer_at(step, me, count)
            if part == 1:
                pl.when(hops(me, peer) > 1)(functools.partial(give, part, peer))
            else:
                give(part, peer)

    for part in range(kinds):
        plane, span = columns(me)
        pltpu.make_async_copy(
            x_ref.at[part, plane, span], wide.at[part, me], in_sem.at[part]
        ).start()

    for load in loads:
        load.wait()
    weights = jnp.concatenate(
        [taps_ref[...], jnp.zeros((3 * reach - taps_ref.shape[0],), jnp.float32)]
    ).reshape(1, 3 * reach)
    taps = weights / jnp.sqrt(jnp.sum(weights * weights))
    tall = jnp.broadcast_to(taps, (16, 3 * reach))
    line = lax.broadcasted_iota(jnp.int32, (16, 3 * reach), 0)
    for bit in range(4):
        tall = jnp.where((line // (1 << bit)) % 2 == 1, pltpu.roll(tall, 1 << bit, 1), tall)

    @pl.loop(0, reach // 16)
    def _(step):
        first = pl.multiple_of(step * 16, 16)
        rolled = pltpu.roll(tall, first, 1)
        band[pl.ds(first, 16), :] = rolled.astype(jnp.bfloat16)

    piece = min(256, width)

    @pl.loop(0, width // piece)
    def _(down):
        @pl.loop(0, width // piece)
        def _(over):
            here = pl.ds(pl.multiple_of(down * piece, piece), piece)
            there = pl.ds(pl.multiple_of(over * piece, piece), piece)
            turned[there, here] = wall[here, there].T

    decay[...] = jnp.exp(-jnp.pi / (2.0 * scale_ref[...]))
    inject[...] = jnp.sqrt(1.0 - jnp.exp(-jnp.pi / scale_ref[...]))

    for part in range(kinds):
        pltpu.make_async_copy(wide.at[part], wide.at[part], in_sem.at[part]).wait()
        share = reach // rows
        for block in range(blocks):
            total = jnp.zeros((reach, slim), jnp.float32)
            for shift in range(3):
                source = (block - 1 + shift) % blocks
                chunk = wide[part, source * share : (source + 1) * share].reshape(reach, slim)
                total += jnp.dot(
                    band[:, shift * reach : (shift + 1) * reach],
                    chunk,
                    preferred_element_type=jnp.float32,
                )
            summed[part, block * share : (block + 1) * share] = total.astype(
                jnp.bfloat16
            ).reshape(share, rows, slim)

        plane, span = columns(me)

        @pl.loop(0, count - 1)
        def _(step):
            peer = peer_at(step, me, count) if part == kinds - 1 else old_peer_at(step, me, count)
            arrival = batch(part, me, peer)
            pltpu.make_async_remote_copy(
                src_ref=summed.at[part, peer],
                dst_ref=back.at[part, plane, span],
                send_sem=back_out_sem.at[part],
                recv_sem=back_in_sem.at[part, arrival],
                device_id=(peer,),
                device_id_type=MESH,
            ).start()

        pltpu.make_async_copy(
            summed.at[part, me], back.at[part, plane, span], back_in_sem.at[part, 0]
        ).start()

    def advance(part, at, filtered):
        one = pl.ds(part, 1)
        state = state_ref[part, :, at]
        states = []
        for plane in range(planes):
            state = decay[one, at] * state + inject[one, at] * filtered[plane]
            states.append(state)
        state_ref[part, :, at] = state
        return states

    def put_along(at, filtered):
        states = advance(0, at, filtered)
        for plane, state in enumerate(states):
            along[plane, :, at] = state
        weave(vel_ref.at[:, 0], mixed, at, [mean_ref[:, at] + diag_ref[0:1, at] * state for state in states])

    def put_normal(at, filtered):
        states = advance(1, at, filtered)
        values = []
        for plane, state in enumerate(states):
            first = along[plane, :, at]
            values.append(off_ref[0:1, at] * first + diag_ref[1:2, at] * state)
            along[plane, :, at] = off_ref[1:2, at] * first + off_ref[2:3, at] * state
        weave(vel_ref.at[:, 1], mixed, at, values)

    def base_spanwise(at, filtered):
        for plane, state in enumerate(advance(2, at, filtered)):
            along[plane, :, at] += diag_ref[2:3, at] * state

    def arrived(part, arrival, pieces):
        piece = wide.at[part, 0:pieces]
        pltpu.make_async_copy(piece, piece, back_in_sem.at[part, arrival]).wait()

    def filtering(part, tile, chunks, early, finish):
        tile = min(tile, width)

        @pl.loop(0, width // tile)
        def _(step):
            at = pl.ds(pl.multiple_of(step * tile, tile), tile)
            total = None
            for first in chunks:
                reading = pl.ds(pl.multiple_of(first * slim, slim), slim)
                term = jnp.dot(
                    back[part, :, first].reshape(planes * rows, slim),
                    turned[reading, at],
                    preferred_element_type=jnp.float32,
                )
                total = term if total is None else total + term
            total = total.reshape(planes, rows, tile)
            if early is not None:
                total += early[:, :, at]
            finish(at, total)

    def keep(early):
        def run(at, filtered):
            early[:, :, at] = filtered

        return run

    ours = me // half
    near = [ours * chips + one for one in range(chips)]
    far = [(1 - ours) * chips + one for one in range(chips)]
    turns = [(me // 2 - late + chips) % chips for late in range(chips)]
    late = [(1 - ours) * chips + turn for turn in turns]
    for at, first in enumerate(late[1:]):
        tail_wall_ref[at * slim : (at + 1) * slim] = turned[
            pl.ds(pl.multiple_of(first * slim, slim), slim)
        ]
    for at, source in enumerate((decay, inject, diag_ref)):
        tail_factors_ref[at : at + 1] = source[2:3]
    arrived(0, 0, count)
    filtering(0, 512, list(range(2 * chips)), None, put_along)
    arrived(1, 0, half)
    filtering(1, 1024, near, None, keep(early_normal))
    arrived(2, 0, half)
    filtering(2, 1024, near, None, keep(early_spanwise))
    arrived(1, 1, half)
    filtering(1, 1024, far, early_normal, put_normal)
    arrived(2, 1, half // chips)
    filtering(2, 1024, late[:1], early_spanwise, base_spanwise)
    arrived(2, 2, half - half // chips)
    for at, first in enumerate(late[1:]):
        tail_ref[:, at * slim : (at + 1) * slim] = back[2, :, first].reshape(planes * rows, slim)

    for part in range(kinds):
        sent = wide.at[part, 0 : count - 1]
        pltpu.make_async_copy(sent, sent, out_sem.at[part]).wait()
        pltpu.make_async_copy(sent, sent, back_out_sem.at[part]).wait()


def store_kernel(
    vel_ref,
    state_ref,
    base_ref,
    tail_ref,
    wall_ref,
    factors_ref,
    vel_out,
    state_out,
    last,
    last_state,
    mixed,
    sem,
):
    planes, rows, width = base_ref.shape
    kinds = state_ref.shape[0]
    ready = pl.ds(0, kinds - 1)
    copies = [
        pltpu.make_async_copy(vel_ref, vel_out.at[:, ready], sem.at[0]),
        pltpu.make_async_copy(state_ref.at[ready], state_out.at[ready], sem.at[1]),
    ]
    for copy in copies:
        copy.start()
    tile = width // CUTS
    for cut in range(CUTS):
        at = pl.ds(cut * tile, tile)
        filtered = jnp.dot(
            tail_ref[...], wall_ref[:, at], preferred_element_type=jnp.float32
        ).reshape(planes, rows, tile)
        decay, inject, diag = (factors_ref[one : one + 1, at] for one in range(3))
        extra = inject * filtered[0]
        values = [base_ref[0, :, at] + diag * extra]
        for plane in range(1, planes):
            extra = decay * extra + inject * filtered[plane]
            values.append(base_ref[plane, :, at] + diag * extra)
        last_state[:, at] = state_ref[kinds - 1, :, at] + extra
        weave(last, mixed, at, values)
        copies += [
            pltpu.make_async_copy(
                last.at[:, :, at], vel_out.at[:, kinds - 1, :, at], sem.at[2 + 2 * cut]
            ),
            pltpu.make_async_copy(
                last_state.at[:, at], state_out.at[kinds - 1, :, at], sem.at[3 + 2 * cut]
            ),
        ]
        for copy in copies[-2:]:
            copy.start()
    for copy in copies:
        copy.wait()


def fits(count, rows, planes, kinds, width, reach, slim):
    return (
        planes * width == count * slim
        and kinds == 3
        and planes == 4
        and count % 16 == 0
        and rows % 16 == 0
        and reach % rows == 0
        and reach % 128 == 0
        and count * rows % reach == 0
        and count * rows // reach >= 3
    )


def exchanged(
    random_slabs,
    span_weights,
    wall_filter,
    prev_state,
    time_scale,
    mean_velocity,
    lund_diag,
    lund_off,
):
    count = lax.axis_size("span")
    rows, planes, kinds, width = random_slabs.shape
    reach = (span_weights.shape[0] - 1) // 2
    slim = LANES
    operands = (
        random_slabs.transpose(0, 2, 1, 3),
        span_weights,
        wall_filter,
        prev_state.transpose(1, 0, 2),
        time_scale,
        mean_velocity.reshape(1, width),
        lund_diag,
        lund_off,
    )
    operands = [pltpu.with_memory_space_constraint(each, pltpu.HBM) for each in operands]
    in_vmem = pl.BlockSpec(memory_space=pltpu.VMEM)
    in_hbm = pl.BlockSpec(memory_space=pltpu.HBM)
    fine = (kinds, width)
    held = pl.pallas_call(
        functools.partial(exchange_kernel, count, rows, width, planes, kinds, slim, reach),
        out_shape=(
            pltpu.VMEM((rows, kinds - 1, planes, width), jnp.bfloat16),
            pltpu.VMEM((kinds, rows, width), jnp.float32),
            pltpu.VMEM((planes, rows, width), jnp.float32),
            pltpu.VMEM((planes * rows, width // 2 - slim), jnp.bfloat16),
            pltpu.VMEM((width // 2 - slim, width), jnp.bfloat16),
            pltpu.VMEM(fine, jnp.float32),
        ),
        in_specs=[in_hbm] * len(operands),
        out_specs=(in_vmem,) * 6,
        scratch_shapes=[
            pltpu.VMEM((kinds, rows, planes, width), jnp.bfloat16),
            pltpu.VMEM(span_weights.shape, jnp.float32),
            pltpu.VMEM(fine, jnp.float32),
            pltpu.VMEM((1, width), jnp.float32),
            pltpu.VMEM(fine, jnp.float32),
            pltpu.VMEM(fine, jnp.float32),
            pltpu.VMEM((kinds, planes, width // slim, rows, slim), jnp.bfloat16),
            pltpu.VMEM((kinds, count, rows, slim), jnp.bfloat16),
            pltpu.VMEM((kinds, count, rows, slim), jnp.bfloat16),
            pltpu.VMEM((kinds, planes, width // slim, rows, slim), jnp.bfloat16),
            pltpu.VMEM((reach, 3 * reach), jnp.bfloat16),
            pltpu.VMEM((width, width), jnp.bfloat16),
            pltpu.VMEM((width, width), jnp.bfloat16),
            pltpu.VMEM((planes, rows, width), jnp.float32),
            pltpu.VMEM((planes, rows, width), jnp.float32),
            pltpu.VMEM(fine, jnp.float32),
            pltpu.VMEM(fine, jnp.float32),
            pltpu.VMEM((width // 128, rows * planes, 128), jnp.float32),
            pltpu.SemaphoreType.DMA((7,)),
            pltpu.SemaphoreType.DMA((kinds,)),
            pltpu.SemaphoreType.DMA((kinds,)),
            pltpu.SemaphoreType.DMA((kinds,)),
            pltpu.SemaphoreType.DMA((kinds,)),
            pltpu.SemaphoreType.DMA((kinds, 3)),
            pltpu.SemaphoreType.REGULAR((count // 8,)),
        ],
        compiler_params=pltpu.CompilerParams(
            collective_id=0, has_side_effects=True, vmem_limit_bytes=GRANT
        ),
    )(*operands)
    velocity, state = pl.pallas_call(
        store_kernel,
        out_shape=(
            jax.ShapeDtypeStruct((rows, kinds, planes, width), jnp.bfloat16),
            jax.ShapeDtypeStruct((kinds, rows, width), jnp.float32),
        ),
        in_specs=[in_vmem] * len(held),
        out_specs=(in_hbm, in_hbm),
        scratch_shapes=[
            pltpu.VMEM((rows, planes, width), jnp.bfloat16),
            pltpu.VMEM((rows, width), jnp.float32),
            pltpu.VMEM((width // 128, rows * planes, 128), jnp.float32),
            pltpu.SemaphoreType.DMA((2 + 2 * CUTS,)),
        ],
        compiler_params=pltpu.CompilerParams(vmem_limit_bytes=GRANT // 2),
    )(*held)
    return velocity.transpose(0, 2, 1, 3), state.transpose(1, 0, 2)


def from_partner(value, axis, bit):
    return lax.ppermute(value, axis, [(i, i ^ 1 << bit) for i in range(lax.axis_size(axis))])


def band_matrix(taps, height):
    reach = taps.shape[0]
    padded = jnp.concatenate([taps, jnp.zeros((height,), taps.dtype)])
    length = reach + height
    tiled = jnp.tile(padded, height)[: height * (length - 1)]
    return tiled.reshape(height, length - 1)


def butterfly(held, forward):
    count = lax.axis_size("span")
    device = lax.axis_index("span")
    levels = count.bit_length() - 1
    for level in range(levels - 1, -1, -1):
        groups, inner_first, targets, inner_last = held.shape
        halves = held.reshape(groups, inner_first, 2, targets // 2, inner_last)
        lower = halves[:, :, 0]
        higher = halves[:, :, 1]
        upper = device >> level & 1 == 1
        kept = jnp.where(upper, higher, lower)
        given = jnp.where(upper, lower, higher)
        if forward:
            taken = from_partner(given, "span", level)
        else:
            taken = from_partner(given, "span", level)
        first = jnp.where(upper, taken, kept)
        second = jnp.where(upper, kept, taken)
        held = jnp.stack([first, second], axis=1).reshape(
            groups * 2, inner_first, targets // 2, inner_last
        )
    return held


def body(
    random_slabs,
    span_weights,
    wall_filter,
    prev_state,
    time_scale,
    mean_velocity,
    lund_diag,
    lund_off,
):
    rows = random_slabs.shape[0]
    planes = random_slabs.shape[1]
    width = random_slabs.shape[3]
    columns = planes * 3 * width
    half = (span_weights.shape[0] - 1) // 2
    if fits(lax.axis_size("span"), rows, planes, 3, width, half, LANES):
        return exchanged(
            random_slabs,
            span_weights,
            wall_filter,
            prev_state,
            time_scale,
            mean_velocity,
            lund_diag,
            lund_off,
        )
    flat = random_slabs.reshape(rows, columns)
    scaling = jnp.sqrt(jnp.sum(span_weights * span_weights))
    taps = (span_weights / scaling).astype(jnp.bfloat16)
    reach = (span_weights.shape[0] - 1) // 2
    count = lax.axis_size("span")
    slim = columns // count
    held = butterfly(flat.reshape(1, rows, count, slim), True)
    total = rows * count
    whole = held.reshape(total, slim)
    height = min(512, total)
    matrix = band_matrix(taps, height)
    wrapped = jnp.concatenate([whole[total - reach :], whole, whole[:reach]], axis=0)

    def one_block(start):
        window = lax.dynamic_slice_in_dim(wrapped, start, height + 2 * reach, 0)
        return jnp.dot(matrix, window, preferred_element_type=jnp.float32)

    starts = jnp.arange(total // height) * height
    summed_cols = lax.map(one_block, starts).reshape(total, slim)
    rounded = summed_cols.astype(jnp.bfloat16)
    returned = butterfly(rounded.reshape(1, 1, count, rows * slim), False)
    spanned = returned.reshape(count, rows, slim).transpose(1, 0, 2).reshape(rows, planes, 3, width)
    filtered = lax.dot_general(
        spanned, wall_filter, (((3,), (1,)), ((), ())), preferred_element_type=jnp.float32
    )
    decay = jnp.exp(-jnp.pi / (2.0 * time_scale))
    inject = jnp.sqrt(1.0 - jnp.exp(-jnp.pi / time_scale))
    state = prev_state
    outputs = []
    for plane in range(planes):
        state = decay * state + inject * filtered[:, plane]
        along = state[:, 0]
        normal = state[:, 1]
        spanwise = state[:, 2]
        first = mean_velocity + lund_diag[0] * along
        second = lund_off[0] * along + lund_diag[1] * normal
        third = lund_off[1] * along + lund_off[2] * normal + lund_diag[2] * spanwise
        outputs.append(jnp.stack([first, second, third], axis=1).astype(jnp.bfloat16))
    velocity = jnp.stack(outputs, axis=1)
    return (velocity, state)


def solution(mesh):
    placed = (P("span", None, None, None), P(), P(), P("span", None, None), P(), P(), P(), P())
    return jax.shard_map(
        body,
        mesh=mesh,
        in_specs=placed,
        out_specs=(P("span", None, None, None), P("span", None, None)),
        check_vma=False,
    )
```
